256 devices in a mesh: dp: 32 (over y, z), group: 8 (over x, core).
Axes of the slice: x: 4, y: 4, z: 8, core: 2. Of those that a mesh axis runs over, the one named last changes fastest.
Arguments:
- keys: int32 [131072], P(('dp', 'group')), may hold values from 0 to 1073741823
- cut: int32 [1], replicated, may hold values from 256 to 1023
- owner: int32 [131072, 1], P(('dp', 'group')), may hold values from 0 to 31; in each aligned block of 512 rows (0 to 511, 512 to 1023, ...) at most 32 rows name the same one
- tokens: int32 [131072, 2048], P(('dp', 'group')), may hold values from 0 to 128255
Outputs:
- histogram: int32 [4096], replicated
- packed_rows: int32 [262144, 2048], P(('dp', 'group'))
- packed_weights: float32 [262144], P(('dp', 'group'))
The draws below stay inside these ranges and needn't reach their ends.
Inputs may be any that keep to these rules, and one draw needn't show every extreme that they name: Among the examples of one device, at most 32 have the same owner, and some owner has exactly 32.
All inputs are finite; a program needn't handle non-finite values.
Results may differ from the reference program's by a relative error of at most 0.0003.
Values sent between devices are 32-bit elements; how exact they have to be, the bound alone decides.
No kernel may reach another device: no remote copies, remote signals or barrier semaphores. Data moves between devices by JAX's collectives and lax.ppermute only.
A program may use at most 128 MiB of HBM per device.

```python
import math
import jax
import jax.numpy as jnp
import numpy as np

EX_DEV = 512
SEQ = 2048
BINS = 4096
BIN_WIDTH = 262144
VOCAB = 128256
EXAMPLES = 131072
MOST = 32
RECV = 1024
N_DP = 32
N_GROUP = 8


def place_ends(array, rng, smallest, top_value):
    extent = array.shape
    place = [jax.random.randint(jax.random.fold_in(rng, axis), (), 0, extent[axis]) for axis in range(len(extent))]
    array = array.at[tuple(place)].set(smallest)
    longest = extent.index(max(extent))
    place[longest] = (place[longest] + 1) % extent[longest]
    return array.at[tuple(place)].set(top_value)


def ranked_wide(rng, extent, amount, slope):
    weights = [min(1 << octave, amount + 1 - (1 << octave)) * (1 << 20) // math.isqrt((1 << octave) ** slope) + 1 for octave in range((amount + 1).bit_length()) if 1 << octave <= amount]
    scale = 1 + sum(weights) // (1 << 30)
    table = np.cumsum(np.array([max(1, weight // scale) for weight in weights]))
    ticket = jax.random.randint(jax.random.fold_in(rng, 1), extent, 0, int(table[len(weights) - 1]))
    start = jnp.left_shift(1, jnp.searchsorted(jnp.asarray(table, jnp.int32), ticket, side="right").astype(jnp.int32))
    rank = start - 1 + jax.random.randint(jax.random.fold_in(rng, 4), extent, 0, 1 << 30) % jnp.minimum(start, amount + 1 - start)
    return jax.random.permutation(jax.random.fold_in(rng, 2), amount)[rank].astype(jnp.int32)


def deal_out(rng, own, number, rows, number_of, top, limit, slope):
    ranking = jax.random.permutation(rng, number_of)
    packed, common = shares(number_of, rows * top, limit, slope, True), shares(number_of, rows * top, limit, slope, False)
    places = jnp.arange(number_of)

    def named(sizes, rotation):
        used = int((sizes > 0).sum())
        fixed = max(1, used // 4)
        moved = fixed + (places - fixed + rotation * (used - fixed)) % max(1, number_of - fixed)
        return jnp.zeros((number_of,), jnp.int32).at[ranking[jnp.where(places < fixed, places, moved)]].set(jnp.asarray(sizes, jnp.int32))

    sizes = jnp.where(number % 4 == 0, named(packed, number // 4), named(common, number - number // 4 - 1))
    mixed = jax.random.permutation(jax.random.fold_in(own, 3), number_of)
    donor, taker = mixed[0:number_of // 2 * 2:2], mixed[1:number_of // 2 * 2:2]
    margin = jnp.minimum(sizes[donor] - 1, limit - sizes[taker]) // 2
    margin = jnp.where((donor == ranking[0]) | (taker == ranking[0]) | (sizes[taker] == 0), 0, jnp.maximum(margin, 0))
    moved = jax.random.randint(jax.random.fold_in(own, 4), (number_of // 2,), 0, 1 << 20) % (margin + 1)
    sizes = sizes.at[donor].add(-moved).at[taker].add(moved)
    members = jnp.searchsorted(jnp.cumsum(sizes), jnp.arange(rows * top), side="right").astype(jnp.int32)
    table = members.reshape(top, rows).T
    table = table[jax.random.permutation(jax.random.fold_in(own, 1), rows)]
    rotation = jax.random.randint(jax.random.fold_in(own, 2), (rows, 1), 0, top)
    return jnp.take_along_axis(table, (jnp.arange(top)[None, :] + rotation) % top, axis=1)


def shares(count, total, bound, slope, full):
    weights = [(1 << 20) // math.isqrt(standing ** slope) + 1 for standing in range(1, count + 1)]
    largest = bound if full else min(bound, max(-(-total // count), total * weights[0] // sum(weights)))
    least = 1 if total - largest >= count - 1 else 0
    counts, spare = [largest] + [least] * (count - 1), total - largest - least * (count - 1)
    while spare > 0:
        free = [i for i in range(1, count) if counts[i] < largest] or [i for i in range(1, count) if counts[i] < bound]
        mass, remaining = sum([weights[i] for i in free]), spare
        for i in free:
            more = min(bound - counts[i], max(1, remaining * weights[i] // mass), spare)
            counts[i] = counts[i] + more
            spare = spare - more
    return np.array(counts)


def setup_inputs(seed: int = 0) -> dict:
    splits = jax.random.split(jax.random.key(seed), 5)
    keys = place_ends(jax.random.randint(splits[0], (EXAMPLES,), 0, BINS * BIN_WIDTH), jax.random.fold_in(splits[0], 1), 0, (BINS * BIN_WIDTH) - 1).astype(jnp.int32)
    cut = jax.random.randint(splits[1], (1,), BINS // 16, BINS // 4).astype(jnp.int32)
    owner_keys = jax.random.split(jax.random.fold_in(splits[2], 1), EXAMPLES // EX_DEV)
    owner_turns = jax.random.permutation(jax.random.fold_in(splits[2], 3), EXAMPLES // EX_DEV)
    owner = jax.vmap(lambda own, number: deal_out(jax.random.fold_in(splits[2], 2), own, number, EX_DEV, N_DP, 1, MOST, 2))(owner_keys, owner_turns).reshape((EXAMPLES, 1))
    tokens = place_ends(ranked_wide(splits[3], (EXAMPLES, SEQ), VOCAB, 2), jax.random.fold_in(splits[3], 3), 0, VOCAB - 1).astype(jnp.int32)
    return {"keys": keys, "cut": cut, "owner": owner, "tokens": tokens}


def reference(keys, cut, owner, tokens):
    bins_of = keys // BIN_WIDTH
    hist = jnp.zeros((BINS,), jnp.float32).at[bins_of].add(1.0)
    kept = bins_of >= cut[0]
    dest = owner[:, 0]
    onehot = ((dest[:, None] == jnp.arange(N_DP, dtype=jnp.int32)[None, :]) & kept[:, None]).astype(jnp.int32)
    running = jnp.cumsum(onehot, axis=0) - onehot
    rank = jnp.sum(running * onehot, axis=1)
    device = dest * N_GROUP + rank % N_GROUP
    slot = rank // N_GROUP
    count = N_DP * N_GROUP * RECV
    target = jnp.where(kept, device * RECV + slot, count).astype(jnp.int32)
    suffix = jnp.cumsum(hist[::-1])[::-1]
    total = jnp.maximum(suffix[cut[0]], 1.0)
    weight = suffix[bins_of] / total
    packed_rows = jnp.zeros((count, SEQ), jnp.int32).at[target].set(tokens, mode="drop")
    packed_weights = jnp.zeros((count,), jnp.float32).at[target].set(weight, mode="drop")
    return hist.astype(jnp.int32), packed_rows, packed_weights
```

```python
import jax
import jax.numpy as jnp
from jax import lax
from jax.experimental import pallas as pl
from jax.experimental.pallas import tpu as pltpu
from jax.sharding import Mesh
from jax.sharding import PartitionSpec as P

BINS = 4096
KEY_SHIFT = 18
DP = ("dp_0", "dp_1")
GROUP = ("group_0", "group_1")
DP_GROUP = ("dp_0", "dp_1", "group_0", "group_1")
LANES = 128
STEP = 64

SMEM = pltpu.MemorySpace.SMEM
VMEM = pltpu.MemorySpace.VMEM


def smem_spec():
    return pl.BlockSpec(memory_space=SMEM)


def any_spec():
    return pl.BlockSpec(memory_space=pl.MemorySpace.ANY)


def pack_rows(keys, dest, info, tokens, n_dev, n_member, slots):
    examples, width = tokens.shape
    tiles = width // LANES
    steps = examples // STEP
    n_owner = n_dev // n_member

    def kernel(keys_ref, dest_ref, info_ref, tok_ref, rows_ref, meta_ref, buf, seen, sent, sem):
        g = pl.program_id(0)

        @pl.when(g == 0)
        def _():
            sent[0] = 0
            for o in range(n_owner):
                seen[o] = 0

        @pl.when(g < steps)
        def _():
            for r in range(STEP // 8):
                for k in range(tiles):
                    at = (g * STEP + r * 8) * tiles + k
                    buf[pl.ds(at, 8, stride=tiles), :] = tok_ref[r * 8 : r * 8 + 8, k * LANES : (k + 1) * LANES]

        @pl.when(g > 0)
        def _():
            lowest = info_ref[0] << KEY_SHIFT

            def row(i, total):
                key = keys_ref[i]
                kept = key >= lowest

                @pl.when(kept)
                def _():
                    o = dest_ref[i]
                    local = seen[o]
                    seen[o] = local + 1
                    member = (info_ref[1 + o] + local) & (n_member - 1)
                    to = (o * n_member + member) * slots + local // n_member
                    meta_ref[to] = key
                    pltpu.make_async_copy(
                        buf.at[pl.ds(pl.multiple_of(i * tiles, tiles), tiles)],
                        rows_ref.at[pl.ds(pl.multiple_of(to * tiles, tiles), tiles)],
                        sem,
                    ).start()

                return total + kept.astype(jnp.int32)

            start = (g - 1) * STEP
            sent[0] = lax.fori_loop(start, start + STEP, row, sent[0])

        @pl.when(g == steps)
        def _():
            def drain(i, carry):
                pltpu.make_async_copy(buf.at[pl.ds(0, tiles)], rows_ref.at[pl.ds(0, tiles)], sem).wait()
                return carry

            lax.fori_loop(0, sent[0], drain, 0)

    return pl.pallas_call(
        kernel,
        grid=(steps + 1,),
        in_specs=[
            smem_spec(),
            smem_spec(),
            smem_spec(),
            pl.BlockSpec((STEP, width), lambda g: (jnp.minimum(g, steps - 1), 0)),
        ],
        out_specs=[any_spec(), smem_spec()],
        out_shape=[
            jax.ShapeDtypeStruct((n_dev * slots * tiles, LANES), tokens.dtype),
            jax.ShapeDtypeStruct((n_dev * slots,), keys.dtype),
        ],
        scratch_shapes=[
            pltpu.VMEM((examples * tiles, LANES), tokens.dtype),
            pltpu.SMEM((n_owner,), jnp.int32),
            pltpu.SMEM((1,), jnp.int32),
            pltpu.SemaphoreType.DMA,
        ],
        name="pack_rows",
    )(keys, dest, info, tokens)


def incoming(counts_ref, member, n_dev, n_member, visit, carry):
    def source(s, state):
        before, carry = state
        count = counts_ref[s]
        first = (member - before) & (n_member - 1)
        rows = (count - first + n_member - 1) >> 3
        carry = visit(s, (before + first) >> 3, rows, carry)
        return before + count, carry

    return lax.fori_loop(0, n_dev, source, (0, carry))


def place_weights(counts, member, got_keys, suffix, n_dev, n_member, slots, capacity):
    def kernel(counts_ref, member_ref, keys_ref, suffix_ref, out_ref):
        def clear(i, carry):
            for j in range(8):
                out_ref[i * 8 + j] = 0.0
            return carry

        lax.fori_loop(0, capacity // 8, clear, 0)

        def visit(s, slot, rows, carry):
            def one(q, c):
                out_ref[slot + q] = suffix_ref[keys_ref[s * slots + q] >> KEY_SHIFT]
                return c

            return lax.fori_loop(0, rows, one, carry)

        incoming(counts_ref, member_ref[0], n_dev, n_member, visit, 0)

    return pl.pallas_call(
        kernel,
        in_specs=[smem_spec()] * 4,
        out_specs=smem_spec(),
        out_shape=jax.ShapeDtypeStruct((capacity,), jnp.float32),
        name="place_weights",
    )(counts, member, got_keys, suffix)


def unpack_rows(counts, member, got, n_dev, n_member, slots, capacity, width):
    tiles = width // LANES
    steps = capacity // STEP

    def kernel(counts_ref, member_ref, got_ref, out_ref, buf, pending, filled, sems):
        g = pl.program_id(0)

        @pl.when(g == 0)
        def _():
            for b in range(steps):
                pending[b] = 0

            def visit(s, slot, rows, carry):
                b = slot // STEP

                @pl.when(rows > 0)
                def _():
                    pending[b] = pending[b] + rows

                for n in range(1, slots + 1):

                    @pl.when(rows == n)
                    def _(n=n):
                        pltpu.make_async_copy(
                            got_ref.at[pl.ds(pl.multiple_of(s * (slots * tiles), tiles), n * tiles)],
                            buf.at[pl.ds(pl.multiple_of(slot * tiles, tiles), n * tiles)],
                            sems.at[b],
                        ).start()

                return carry

            total, _ = incoming(counts_ref, member_ref[0], n_dev, n_member, visit, 0)
            filled[0] = (total - member_ref[0] + n_member - 1) >> 3

        def drain(i, carry):
            pltpu.make_async_copy(got_ref.at[pl.ds(0, tiles)], buf.at[pl.ds(0, tiles)], sems.at[g]).wait()
            return carry

        lax.fori_loop(0, pending[g], drain, 0)
        index = g * STEP + lax.broadcasted_iota(jnp.int32, (8, LANES), 0)
        for r in range(STEP // 8):
            real = index + r * 8 < filled[0]
            for k in range(tiles):
                at = (g * STEP + r * 8) * tiles + k
                rows = buf[pl.ds(at, 8, stride=tiles), :]
                out_ref[r * 8 : r * 8 + 8, k * LANES : (k + 1) * LANES] = jnp.where(real, rows, 0)

    return pl.pallas_call(
        kernel,
        grid=(steps,),
        in_specs=[smem_spec(), smem_spec(), any_spec()],
        out_specs=pl.BlockSpec((STEP, width), lambda g: (g, 0)),
        out_shape=jax.ShapeDtypeStruct((capacity, width), got.dtype),
        scratch_shapes=[
            pltpu.VMEM((capacity * tiles, LANES), got.dtype),
            pltpu.SMEM((steps,), jnp.int32),
            pltpu.SMEM((1,), jnp.int32),
            pltpu.SemaphoreType.DMA((steps,)),
        ],
        name="unpack_rows",
    )(counts, member, got)


def exchange(value):
    return lax.all_to_all(value, DP_GROUP, split_axis=0, concat_axis=0, tiled=True)


def body(keys, cut, owner, tokens):
    examples = keys.shape[0]
    width = tokens.shape[1]
    n_owner = lax.axis_size(DP)
    n_member = lax.axis_size(GROUP)
    n_dev = n_owner * n_member
    slots = 2 * examples // n_dev
    capacity = 2 * examples
    piece = BINS // n_dev
    me = lax.axis_index(DP_GROUP)
    member = lax.axis_index(GROUP)
    bins_of = keys >> KEY_SHIFT
    dest = owner[:, 0]
    kept = bins_of >= cut[0]
    owners = jnp.arange(n_owner, dtype=jnp.int32)
    counts = jnp.sum(((dest[:, None] == owners[None, :]) & kept[:, None]).astype(jnp.int32), axis=0)
    local_hist = jnp.zeros((BINS,), jnp.int32).at[bins_of].add(1)
    first = jnp.concatenate(
        [local_hist.reshape(n_dev, piece), jnp.broadcast_to(counts[None, :], (n_dev, n_owner))], axis=1
    )
    first = exchange(first)
    piece_sum = jnp.sum(first[:, :piece], axis=0)
    table = first[:, piece:]
    earlier = jnp.arange(n_dev, dtype=jnp.int32)[:, None] < me
    before = jnp.sum(jnp.where(earlier, table, 0), axis=0)
    mine = lax.dynamic_slice_in_dim(table, me // n_member, 1, axis=1)[:, 0]
    info = jnp.concatenate([cut, before])
    send_rows, send_keys = pack_rows(keys, dest, info, tokens, n_dev, n_member, slots)
    second = jnp.concatenate(
        [send_keys.reshape(n_dev, slots), jnp.broadcast_to(piece_sum[None, :], (n_dev, piece))], axis=1
    )
    second = exchange(second)
    got_keys = second[:, :slots].reshape(-1)
    hist = second[:, slots:].reshape(-1)
    got = exchange(send_rows.reshape(n_dev, slots, width // LANES, LANES)).reshape(-1, LANES)
    suffix = jnp.cumsum(hist.astype(jnp.float32)[::-1])[::-1]
    total = jnp.maximum(suffix[cut[0]], 1.0)
    member = member[None].astype(jnp.int32)
    weights = place_weights(mine, member, got_keys, suffix, n_dev, n_member, slots, capacity) / total
    packed = unpack_rows(mine, member, got, n_dev, n_member, slots, capacity, width)
    return (hist, packed, weights)


def solution(mesh):
    torus = Mesh(mesh.devices.reshape(4, 8, 4, 2), ("dp_0", "dp_1", "group_0", "group_1"))
    placed = (P(DP_GROUP), P(), P(DP_GROUP, None), P(DP_GROUP, None))
    return jax.shard_map(
        body,
        mesh=torus,
        in_specs=placed,
        out_specs=(P(), P(DP_GROUP, None), P(DP_GROUP)),
        check_vma=False,
    )
```

```python
import jax
import jax.numpy as jnp
from jax import lax
from jax.experimental import pallas as pl
from jax.experimental.pallas import tpu as pltpu
from jax.sharding import Mesh
from jax.sharding import PartitionSpec as P


BINS = 4096
KEY_SHIFT = 18
DP = ("dp_0", "dp_1")
GROUP = ("group_0", "group_1")
DP_GROUP = ("dp_0", "dp_1", "group_0", "group_1")
LANES = 128
STEP = 64

SMEM = pltpu.MemorySpace.SMEM


def smem_spec():
    return pl.BlockSpec(memory_space=SMEM)


def any_spec():
    return pl.BlockSpec(memory_space=pltpu.MemorySpace.HBM)


def pack_rows(keys, dest, info, tokens, n_dev, n_member, slots):
    examples, width = tokens.shape
    tiles = width // LANES
    steps = examples // STEP
    n_owner = n_dev // n_member

    def kernel(keys_ref, dest_ref, info_ref, tok_ref, rows_ref, meta_ref, buf, seen, sent, sem):
        g = pl.program_id(0)

        @pl.when(g == 0)
        def _():
            sent[0] = 0
            for o in range(n_owner):
                seen[o] = 0

        @pl.when(g < steps)
        def _():
            for r in range(STEP // 8):
                for k in range(tiles):
                    at = (g * STEP + r * 8) * tiles + k
                    buf[pl.ds(at, 8, stride=tiles), :] = tok_ref[r * 8 : r * 8 + 8, k * LANES : (k + 1) * LANES]

        @pl.when(g > 0)
        def _():
            lowest = info_ref[0] << KEY_SHIFT

            def row(i, total):
                key = keys_ref[i]
                kept = key >= lowest

                @pl.when(kept)
                def _():
                    o = dest_ref[i]
                    local = seen[o]
                    seen[o] = local + 1
                    member = (info_ref[1 + o] + local) & (n_member - 1)
                    to = (o * n_member + member) * slots + local // n_member
                    meta_ref[to] = key
                    pltpu.make_async_copy(
                        buf.at[pl.ds(pl.multiple_of(i * tiles, tiles), tiles)],
                        rows_ref.at[pl.ds(pl.multiple_of(to * tiles, tiles), tiles)],
                        sem,
                    ).start()

                return total + kept.astype(jnp.int32)

            start = (g - 1) * STEP
            sent[0] = lax.fori_loop(start, start + STEP, row, sent[0])

        @pl.when(g == steps)
        def _():
            def drain(i, carry):
                pltpu.make_async_copy(buf.at[pl.ds(0, tiles)], rows_ref.at[pl.ds(0, tiles)], sem).wait()
                return carry

            lax.fori_loop(0, sent[0], drain, 0)

    return pl.pallas_call(
        kernel,
        grid=(steps + 1,),
        in_specs=[
            smem_spec(),
            smem_spec(),
            smem_spec(),
            pl.BlockSpec((STEP, width), lambda g: (jnp.minimum(g, steps - 1), 0)),
        ],
        out_specs=[any_spec(), smem_spec()],
        out_shape=[
            jax.ShapeDtypeStruct((n_dev * slots * tiles, LANES), tokens.dtype),
            jax.ShapeDtypeStruct((n_dev * slots,), keys.dtype),
        ],
        scratch_shapes=[
            pltpu.VMEM((examples * tiles, LANES), tokens.dtype),
            pltpu.SMEM((n_owner,), jnp.int32),
            pltpu.SMEM((1,), jnp.int32),
            pltpu.SemaphoreType.DMA,
        ],
        name="pack_rows",
    )(keys, dest, info, tokens)


def incoming(counts_ref, member, n_dev, n_member, visit, carry):
    def source(s, state):
        before, carry = state
        count = counts_ref[s]
        first = (member - before) & (n_member - 1)
        rows = (count - first + n_member - 1) >> 3
        carry = visit(s, (before + first) >> 3, rows, carry)
        return before + count, carry

    return lax.fori_loop(0, n_dev, source, (0, carry))


def place_weights(counts, member, got_keys, suffix, n_dev, n_member, slots, capacity):
    def kernel(counts_ref, member_ref, keys_ref, suffix_ref, out_ref):
        def clear(i, carry):
            for j in range(8):
                out_ref[i * 8 + j] = 0.0
            return carry

        lax.fori_loop(0, capacity // 8, clear, 0)

        def visit(s, slot, rows, carry):
            def one(q, c):
                out_ref[slot + q] = suffix_ref[keys_ref[s * slots + q] >> KEY_SHIFT]
                return c

            return lax.fori_loop(0, rows, one, carry)

        incoming(counts_ref, member_ref[0], n_dev, n_member, visit, 0)

    return pl.pallas_call(
        kernel,
        in_specs=[smem_spec()] * 4,
        out_specs=smem_spec(),
        out_shape=jax.ShapeDtypeStruct((capacity,), jnp.float32),
        name="place_weights",
    )(counts, member, got_keys, suffix)


def unpack_rows(counts, member, got, n_dev, n_member, slots, capacity, width):
    tiles = width // LANES
    steps = capacity // STEP

    def kernel(counts_ref, member_ref, got_ref, out_ref, buf, pending, filled, sems):
        g = pl.program_id(0)

        @pl.when(g == 0)
        def _():
            for b in range(steps):
                pending[b] = 0

            def visit(s, slot, rows, carry):
                b = slot // STEP

                @pl.when(rows > 0)
                def _():
                    pending[b] = pending[b] + rows

                for n in range(1, slots + 1):

                    @pl.when(rows == n)
                    def _(n=n):
                        pltpu.make_async_copy(
                            got_ref.at[pl.ds(pl.multiple_of(s * (slots * tiles), tiles), n * tiles)],
                            buf.at[pl.ds(pl.multiple_of(slot * tiles, tiles), n * tiles)],
                            sems.at[b],
                        ).start()

                return carry

            total, _ = incoming(counts_ref, member_ref[0], n_dev, n_member, visit, 0)
            filled[0] = (total - member_ref[0] + n_member - 1) >> 3

        def drain(i, carry):
            pltpu.make_async_copy(got_ref.at[pl.ds(0, tiles)], buf.at[pl.ds(0, tiles)], sems.at[g]).wait()
            return carry

        lax.fori_loop(0, pending[g], drain, 0)
        index = g * STEP + lax.broadcasted_iota(jnp.int32, (8, LANES), 0)
        for r in range(STEP // 8):
            real = index + r * 8 < filled[0]
            for k in range(tiles):
                at = (g * STEP + r * 8) * tiles + k
                rows = buf[pl.ds(at, 8, stride=tiles), :]
                out_ref[r * 8 : r * 8 + 8, k * LANES : (k + 1) * LANES] = jnp.where(real, rows, 0)

    return pl.pallas_call(
        kernel,
        grid=(steps,),
        in_specs=[smem_spec(), smem_spec(), any_spec()],
        out_specs=pl.BlockSpec((STEP, width), lambda g: (g, 0)),
        out_shape=jax.ShapeDtypeStruct((capacity, width), got.dtype),
        scratch_shapes=[
            pltpu.VMEM((capacity * tiles, LANES), got.dtype),
            pltpu.SMEM((steps,), jnp.int32),
            pltpu.SMEM((1,), jnp.int32),
            pltpu.SemaphoreType.DMA((steps,)),
        ],
        name="unpack_rows",
    )(counts, member, got)


CAPS = (288, 216, 144, 56)
OWN = 128


def segments(k):
    edges = (0,) + CAPS[::-1]
    return [(edges[j], edges[j + 1] - edges[j]) for j in range(5 - k)]


def pack_relay(source, tokens):
    examples, width = tokens.shape
    tiles = width // LANES
    steps = examples // STEP
    sizes = [n for _, n in segments(1)] * 2 + [OWN]

    def kernel(source_ref, tok_ref, *rest):
        outs, (buf, sem) = rest[: len(sizes)], rest[len(sizes) :]
        g = pl.program_id(0)

        @pl.when(g < steps)
        def _():
            for r in range(STEP // 8):
                for k in range(tiles):
                    at = (g * STEP + r * 8) * tiles + k
                    buf[pl.ds(at, 8, stride=tiles), :] = tok_ref[r * 8 : r * 8 + 8, k * LANES : (k + 1) * LANES]

        @pl.when(g == steps)
        def _():
            start = 0
            for out, size in zip(outs, sizes):

                def some(i, carry, out=out, start=start):
                    for j in range(8):
                        p = i * 8 + j
                        row = source_ref[start + p]
                        pltpu.make_async_copy(
                            buf.at[pl.ds(pl.multiple_of(row * tiles, tiles), tiles)],
                            out.at[pl.ds(pl.multiple_of(p * tiles, tiles), tiles)],
                            sem,
                        ).start()
                    return carry

                lax.fori_loop(0, size // 8, some, 0)
                start += size
            for out, size in zip(outs, sizes):
                pltpu.make_async_copy(buf.at[pl.ds(0, size * tiles)], out, sem).wait()

    return pl.pallas_call(
        kernel,
        grid=(steps + 1,),
        in_specs=[smem_spec(), pl.BlockSpec((STEP, width), lambda g: (jnp.minimum(g, steps - 1), 0))],
        out_specs=[any_spec()] * len(sizes),
        out_shape=[jax.ShapeDtypeStruct((n * tiles, LANES), tokens.dtype) for n in sizes],
        scratch_shapes=[pltpu.VMEM((examples * tiles, LANES), tokens.dtype), pltpu.SemaphoreType.DMA],
        name="pack_relay",
    )(source, tokens)


ROUNDS = ((0, 1), (2,), (3, 4))


def lanes_of(hop):
    if hop == 0:
        return [((0,), 4)]
    if hop == 4:
        return [((0, 1), 4)]
    return [((0,), 4), ((1,), 4)]


def slot_map():
    found = {}
    for n, hops in enumerate(ROUNDS):
        skip = 0
        for hop in hops:
            for sides, slots in lanes_of(hop):
                for side in sides:
                    found[hop if side == 0 else (8 - hop) % 8] = (n, skip)
                skip += slots
        for d, (m, at) in list(found.items()):
            if m == n and not isinstance(at, tuple):
                found[d] = (m, (at, skip))
    return {d: (n, rows, at) for d, (n, (at, rows)) in found.items()}


def spread(n, place, counts, befores, pieces, n_member, tiles):
    slots = slot_map()
    width = next(rows for m, rows, _ in slots.values() if m == n)
    total = 4 * n_member * width * tiles
    origins, held = {}, 0
    for hop, side, start, rows, _ in pieces:
        if (hop, side) not in origins:
            rows_in = OWN if hop == 0 else CAPS[hop - 1]
            origins[hop, side] = (held, rows_in)
            held += rows_in + 32
    arrays = [array for *_, array in pieces]

    def kernel(place_ref, counts_ref, befores_ref, *rest):
        ins, (out, buf, sem_in, sem_out) = rest[: len(pieces)], rest[len(pieces) :]
        loads = []
        for (hop, side, start, rows, _), ref in zip(pieces, ins):
            at = (origins[hop, side][0] + start) * tiles
            loads.append(pltpu.make_async_copy(ref, buf.at[pl.ds(at, rows * tiles)], sem_in))
        for load in loads:
            load.start()
        z = place_ref[0]
        todo = []
        for (hop, side), (base, rows_in) in origins.items():
            sign = 1 - 2 * side
            origin = (z - sign * hop) & 7

            def share(y, k, origin=origin, sign=sign, side=side):
                count = counts_ref[origin * 32 + y * 8 + ((origin + sign * k) & 7)]
                return (count + 1 - side) >> 1 if k == 4 else count

            at = 0
            if hop > 0:
                for k in range(hop + 1, 5):
                    for y in range(4):
                        at += share(y, k)
            for y in range(4):
                todo.append((hop, side, y, base + jnp.minimum(at, rows_in), befores_ref[origin * 32 + y * 8 + z]))
                at += share(y, hop)
        for load in loads:
            load.wait()
        for hop, side, y, first, before in todo:
            skip = slots[hop if side == 0 else (8 - hop) % 8][2]
            for j in range(16 if hop == 4 else 32):
                local = 2 * j + side if hop == 4 else j
                member = (before + local) & (n_member - 1)
                to = (y * n_member + member) * width + skip + local // n_member
                pltpu.make_async_copy(
                    buf.at[pl.ds(pl.multiple_of((first + j) * tiles, tiles), tiles)],
                    out.at[pl.ds(pl.multiple_of(to * tiles, tiles), tiles)],
                    sem_out,
                ).start()
        pltpu.make_async_copy(buf.at[pl.ds(0, total)], out, sem_out).wait()

    return pl.pallas_call(
        kernel,
        in_specs=[smem_spec()] * 3 + [any_spec()] * len(pieces),
        out_specs=any_spec(),
        out_shape=jax.ShapeDtypeStruct((total, LANES), arrays[0].dtype),
        scratch_shapes=[
            pltpu.VMEM((max(held * tiles, total), LANES), arrays[0].dtype),
            pltpu.SemaphoreType.DMA,
            pltpu.SemaphoreType.DMA,
        ],
    )(place, counts, befores, *arrays)


def unpack_relay(place, counts, befores, got, n_member, capacity, width):
    tiles = width // LANES
    steps = capacity // STEP
    slots = 4
    where = slot_map()

    def kernel(place_ref, counts_ref, befores_ref, *rest):
        ins, (out_ref, buf, pending, sems) = rest[: len(got)], rest[len(got) :]
        g = pl.program_id(0)
        z, member = place_ref[0], place_ref[1]
        last = 32 * n_member - 1
        filled = (befores_ref[last] + counts_ref[last] - member + n_member - 1) >> 3

        @pl.when(g == 0)
        def _():
            for b in range(steps):
                pending[b] = 0
            for d in range(8):
                n, rows_each, skip = where[d]
                ref = ins[n]
                origin = (z - d) & 7

                def sender(i, carry, ref=ref, rows_each=rows_each, skip=skip, origin=origin):
                    s = ((i >> 3) * 8 + origin) * n_member + (i & 7)
                    before = befores_ref[s]
                    first = (member - before) & (n_member - 1)
                    rows = (counts_ref[s] - first + n_member - 1) >> 3
                    slot = (before + first) >> 3
                    b = slot // STEP
                    at = i * rows_each + skip

                    @pl.when(rows > 0)
                    def _():
                        pending[b] = pending[b] + rows

                    for n in range(1, slots + 1):

                        @pl.when(rows == n)
                        def _(n=n):
                            pltpu.make_async_copy(
                                ref.at[pl.ds(pl.multiple_of(at * tiles, tiles), n * tiles)],
                                buf.at[pl.ds(pl.multiple_of(slot * tiles, tiles), n * tiles)],
                                sems.at[b],
                            ).start()

                    return carry

                lax.fori_loop(0, 4 * n_member, sender, 0)

        def drain(i, carry):
            pltpu.make_async_copy(ins[0].at[pl.ds(0, tiles)], buf.at[pl.ds(0, tiles)], sems.at[g]).wait()
            return carry

        lax.fori_loop(0, pending[g], drain, 0)
        index = g * STEP + lax.broadcasted_iota(jnp.int32, (8, LANES), 0)
        for r in range(STEP // 8):
            real = index + r * 8 < filled
            for k in range(tiles):
                at = (g * STEP + r * 8) * tiles + k
                rows = buf[pl.ds(at, 8, stride=tiles), :]
                out_ref[r * 8 : r * 8 + 8, k * LANES : (k + 1) * LANES] = jnp.where(real, rows, 0)

    return pl.pallas_call(
        kernel,
        grid=(steps,),
        in_specs=[smem_spec()] * 3 + [any_spec()] * len(got),
        out_specs=pl.BlockSpec((STEP, width), lambda g: (g, 0)),
        out_shape=jax.ShapeDtypeStruct((capacity, width), got[0].dtype),
        scratch_shapes=[
            pltpu.VMEM((capacity * tiles, LANES), got[0].dtype),
            pltpu.SMEM((steps,), jnp.int32),
            pltpu.SemaphoreType.DMA((steps,)),
        ],
        name="unpack_relay",
    )(place, counts, befores, *got)


def relay_source(counts, local_rank, onehot, z):
    owner = jnp.arange(32, dtype=jnp.int32)
    y, d = owner // 8, (owner - z) % 8
    dist = jnp.minimum(d, 8 - d)
    order = (4 - dist) * 4 + y
    plus = (d >= 1) & (d <= 4)
    minus = d >= 4
    own = d == 0
    size_plus = jnp.where(d == 4, (counts + 1) >> 1, counts)
    size_minus = jnp.where(d == 4, counts >> 1, counts)
    earlier = order[None, :] < order[:, None]

    def start(members, sizes):
        return jnp.sum(jnp.where(earlier & members[None, :], sizes[None, :], 0), axis=1)

    side = CAPS[0]
    base = jnp.where(own, 2 * side + start(own, counts), jnp.where(plus, start(plus, size_plus), side + start(minus, size_minus)))
    other = side + start(minus, size_minus)
    limit = jnp.where(own, 2 * side + OWN, jnp.where(plus, side, 2 * side))

    def pick(values):
        return jnp.sum(onehot * values[None, :], axis=1)

    four = pick((d == 4).astype(jnp.int32)) == 1
    odd = four & ((local_rank & 1) == 1)
    position = jnp.where(odd, pick(other), pick(base)) + jnp.where(four, local_rank >> 1, local_rank)
    bound = jnp.where(odd, 2 * side, pick(limit))
    position = jnp.where((jnp.sum(onehot, axis=1) == 1) & (position < bound), position, -1)
    example = jnp.arange(onehot.shape[0], dtype=jnp.int32)
    places = jnp.arange(2 * side + OWN, dtype=jnp.int32)
    return jnp.sum(jnp.where(position[None, :] == places[:, None], example[None, :], 0), axis=1)


def relay_fits(table):
    n_dev = table.shape[0]
    z = (jnp.arange(n_dev, dtype=jnp.int32)[:, None] // 8) % 8
    d = (jnp.arange(32, dtype=jnp.int32)[None, :] - z) % 8
    plus = jnp.where(d == 4, (table + 1) >> 1, table)
    over = jnp.zeros((), jnp.int32)
    for k, cap in enumerate(CAPS, 1):
        ahead = jnp.sum(jnp.where((d >= k) & (d <= 4), plus, 0), axis=1)
        behind = jnp.sum(jnp.where((d <= 8 - k) & (d >= 4), jnp.where(d == 4, table >> 1, table), 0), axis=1)
        over = jnp.maximum(over, jnp.max(jnp.maximum(ahead, behind)) - cap)
    return over <= 0


def exchange(value, axes=DP_GROUP):
    return lax.all_to_all(value, axes, split_axis=0, concat_axis=0, tiled=True)


def hop_on(value, step):
    count = lax.axis_size("dp_1")
    return lax.ppermute(value, "dp_1", [(i, (i + step) % count) for i in range(count)])


def program(keys, cut, owner, tokens):
    examples = keys.shape[0]
    width = tokens.shape[1]
    tiles = width // LANES
    n_owner = lax.axis_size(DP)
    n_member = lax.axis_size(GROUP)
    n_dev = n_owner * n_member
    slots = 2 * examples // n_dev
    capacity = 2 * examples
    piece = BINS // n_dev
    me = lax.axis_index(DP_GROUP)
    member = lax.axis_index(GROUP)
    y, z = lax.axis_index("dp_0"), lax.axis_index("dp_1")
    bins_of = keys >> KEY_SHIFT
    dest = owner[:, 0]
    kept = bins_of >= cut[0]
    owners = jnp.arange(n_owner, dtype=jnp.int32)
    onehot = ((dest[:, None] == owners[None, :]) & kept[:, None]).astype(jnp.int32)
    counts = jnp.sum(onehot, axis=0)
    index = jnp.arange(examples, dtype=jnp.int32)
    lower = (index[None, :] < index[:, None]).astype(jnp.bfloat16)
    running = jnp.dot(lower, onehot.astype(jnp.bfloat16), preferred_element_type=jnp.float32).astype(jnp.int32)
    local_rank = jnp.sum(running * onehot, axis=1)
    source = relay_source(counts, local_rank, onehot, z)
    *pieces, own = pack_relay(source, tokens)
    plus, minus = pieces[:4], pieces[4:]

    local_hist = jnp.zeros((BINS,), jnp.int32).at[bins_of].add(1)
    first = jnp.concatenate(
        [local_hist.reshape(n_dev, piece), jnp.broadcast_to(counts[None, :], (n_dev, n_owner))], axis=1
    )
    first, _ = lax.optimization_barrier((first, source))
    first = exchange(first)
    piece_sum = jnp.sum(first[:, :piece], axis=0)
    table = first[:, piece:]
    device = jnp.arange(n_dev, dtype=jnp.int32)
    below = (device[None, :] < device[:, None]).astype(jnp.bfloat16)
    befores = jnp.dot(below, table.astype(jnp.bfloat16), preferred_element_type=jnp.float32).astype(jnp.int32)
    before = lax.dynamic_slice_in_dim(befores, me, 1, axis=0)[0]

    def column(values):
        return lax.dynamic_slice_in_dim(values, me // n_member, 1, axis=1)[:, 0]

    def line(values):
        return lax.dynamic_slice(values.reshape(4, 8, n_member, n_owner), (y, 0, member, 0), (1, 8, 1, n_owner)).reshape(-1)

    mine, mine_before = column(table), column(befores)
    line_counts, line_befores = line(table), line(befores)
    fits = relay_fits(table)
    place = jnp.stack([z, member]).astype(jnp.int32)

    late_keys, late_dest, before = lax.optimization_barrier((keys, dest, before))
    late_kept = late_keys >> KEY_SHIFT >= cut[0]
    late = (late_dest[:, None] == owners[None, :]) & late_kept[:, None]
    rank = jnp.sum(jnp.where(late, before[None, :], 0), axis=1) + local_rank
    to = jnp.where(late_kept, (dest * n_member + rank % n_member) * slots + local_rank // n_member, n_dev * slots)
    send_keys = jnp.zeros((n_dev * slots,), jnp.int32).at[to].set(keys, mode="drop")
    second = jnp.concatenate(
        [send_keys.reshape(n_dev, slots), jnp.broadcast_to(piece_sum[None, :], (n_dev, piece))], axis=1
    )
    second = exchange(second)
    arrived = {0: [(0, 0, 0, OWN, own)]}
    for k in range(1, 5):
        plus = [hop_on(v, 1) for v in plus[: 5 - k]]
        minus = [hop_on(v, -1) for v in minus[: 5 - k]]
        arrived[k] = [(k, i, *span, v) for i, side in enumerate((plus, minus)) for span, v in zip(segments(k), side)]
    got = []
    for n, hops in enumerate(ROUNDS):
        laid = spread(n, place, line_counts, line_befores, [p for k in hops for p in arrived[k]], n_member, tiles)
        laid = laid.reshape(n_owner, -1, tiles, LANES)
        if n == 0:
            laid, second = lax.optimization_barrier((laid, second))
        else:
            laid, got[-1] = lax.optimization_barrier((laid, got[-1]))
        got.append(exchange(laid, ("dp_0",) + GROUP).reshape(-1, LANES))

    got_keys = second[:, :slots].reshape(-1)
    hist = second[:, slots:].reshape(-1)
    suffix = jnp.cumsum(hist.astype(jnp.float32)[::-1])[::-1]
    total = jnp.maximum(suffix[cut[0]], 1.0)
    weights = place_weights(mine, member[None], got_keys, suffix, n_dev, n_member, slots, capacity) / total

    def relayed(got):
        return unpack_relay(place, mine, mine_before, got, n_member, capacity, width)

    def direct(got):
        info = jnp.concatenate([cut, before])
        send_rows, _ = pack_rows(keys, dest, info, tokens, n_dev, n_member, slots)
        rows = exchange(send_rows.reshape(n_dev, slots, tiles, LANES)).reshape(-1, LANES)
        return unpack_rows(mine, member[None], rows, n_dev, n_member, slots, capacity, width)

    packed = lax.cond(fits, relayed, direct, got)
    return (hist, packed, weights)


def solution(mesh):
    torus = Mesh(mesh.devices.reshape(4, 8, 4, 2), ("dp_0", "dp_1", "group_0", "group_1"))
    placed = (P(DP_GROUP), P(), P(DP_GROUP, None), P(DP_GROUP, None))
    return jax.shard_map(
        program,
        mesh=torus,
        in_specs=placed,
        out_specs=(P(), P(DP_GROUP, None), P(DP_GROUP)),
        check_vma=False,
    )
```

```python
import jax
import jax.numpy as jnp
from jax import lax
from jax.experimental import pallas as pl
from jax.experimental.pallas import tpu as pltpu
from jax.sharding import Mesh
from jax.sharding import PartitionSpec as P


BINS = 4096
KEY_SHIFT = 18
DP = ("dp_0", "dp_1")
GROUP = ("group_0", "group_1")
DP_GROUP = ("dp_0", "dp_1", "group_0", "group_1")
LANES = 128
STEP = 64

SMEM = pltpu.MemorySpace.SMEM


def smem_spec():
    return pl.BlockSpec(memory_space=SMEM)


def any_spec():
    return pl.BlockSpec(memory_space=pltpu.MemorySpace.HBM)


def pack_rows(keys, dest, info, tokens, n_dev, n_member, slots):
    examples, width = tokens.shape
    tiles = width // LANES
    steps = examples // STEP
    n_owner = n_dev // n_member

    def kernel(keys_ref, dest_ref, info_ref, tok_ref, rows_ref, meta_ref, buf, seen, sent, sem):
        g = pl.program_id(0)

        @pl.when(g == 0)
        def _():
            sent[0] = 0
            for o in range(n_owner):
                seen[o] = 0

        @pl.when(g < steps)
        def _():
            for r in range(STEP // 8):
                for k in range(tiles):
                    at = (g * STEP + r * 8) * tiles + k
                    buf[pl.ds(at, 8, stride=tiles), :] = tok_ref[r * 8 : r * 8 + 8, k * LANES : (k + 1) * LANES]

        @pl.when(g > 0)
        def _():
            lowest = info_ref[0] << KEY_SHIFT

            def row(i, total):
                key = keys_ref[i]
                kept = key >= lowest

                @pl.when(kept)
                def _():
                    o = dest_ref[i]
                    local = seen[o]
                    seen[o] = local + 1
                    member = (info_ref[1 + o] + local) & (n_member - 1)
                    to = (o * n_member + member) * slots + local // n_member
                    meta_ref[to] = key
                    pltpu.make_async_copy(
                        buf.at[pl.ds(pl.multiple_of(i * tiles, tiles), tiles)],
                        rows_ref.at[pl.ds(pl.multiple_of(to * tiles, tiles), tiles)],
                        sem,
                    ).start()

                return total + kept.astype(jnp.int32)

            start = (g - 1) * STEP
            sent[0] = lax.fori_loop(start, start + STEP, row, sent[0])

        @pl.when(g == steps)
        def _():
            def drain(i, carry):
                pltpu.make_async_copy(buf.at[pl.ds(0, tiles)], rows_ref.at[pl.ds(0, tiles)], sem).wait()
                return carry

            lax.fori_loop(0, sent[0], drain, 0)

    return pl.pallas_call(
        kernel,
        grid=(steps + 1,),
        in_specs=[
            smem_spec(),
            smem_spec(),
            smem_spec(),
            pl.BlockSpec((STEP, width), lambda g: (jnp.minimum(g, steps - 1), 0)),
        ],
        out_specs=[any_spec(), smem_spec()],
        out_shape=[
            jax.ShapeDtypeStruct((n_dev * slots * tiles, LANES), tokens.dtype),
            jax.ShapeDtypeStruct((n_dev * slots,), keys.dtype),
        ],
        scratch_shapes=[
            pltpu.VMEM((examples * tiles, LANES), tokens.dtype),
            pltpu.SMEM((n_owner,), jnp.int32),
            pltpu.SMEM((1,), jnp.int32),
            pltpu.SemaphoreType.DMA,
        ],
        name="pack_rows",
    )(keys, dest, info, tokens)


def incoming(counts_ref, member, n_dev, n_member, visit, carry):
    def source(s, state):
        before, carry = state
        count = counts_ref[s]
        first = (member - before) & (n_member - 1)
        rows = (count - first + n_member - 1) >> 3
        carry = visit(s, (before + first) >> 3, rows, carry)
        return before + count, carry

    return lax.fori_loop(0, n_dev, source, (0, carry))


def place_bins(counts, member, got_keys, n_dev, n_member, slots, capacity):
    def kernel(counts_ref, member_ref, keys_ref, out_ref):
        def clear(i, carry):
            for j in range(8):
                out_ref[i * 8 + j] = -1
            return carry

        lax.fori_loop(0, capacity // 8, clear, 0)

        def visit(s, slot, rows, carry):
            at = s * (slots * n_member) + ((member_ref[0] - carry) & (n_member - 1))

            def one(q, c):
                out_ref[slot + q] = keys_ref[at + q * n_member] >> KEY_SHIFT
                return c

            lax.fori_loop(0, rows, one, 0)
            return carry + counts_ref[s]

        incoming(counts_ref, member_ref[0], n_dev, n_member, visit, 0)

    return pl.pallas_call(
        kernel,
        in_specs=[smem_spec()] * 3,
        out_specs=smem_spec(),
        out_shape=jax.ShapeDtypeStruct((capacity,), jnp.int32),
        name="place_bins",
    )(counts, member, got_keys)


def unpack_rows(counts, member, got, n_dev, n_member, slots, capacity, width):
    tiles = width // LANES
    steps = capacity // STEP

    def kernel(counts_ref, member_ref, got_ref, out_ref, buf, pending, filled, sems):
        g = pl.program_id(0)

        @pl.when(g == 0)
        def _():
            for b in range(steps):
                pending[b] = 0

            def visit(s, slot, rows, carry):
                b = slot // STEP

                @pl.when(rows > 0)
                def _():
                    pending[b] = pending[b] + rows

                for n in range(1, slots + 1):

                    @pl.when(rows == n)
                    def _(n=n):
                        pltpu.make_async_copy(
                            got_ref.at[pl.ds(pl.multiple_of(s * (slots * tiles), tiles), n * tiles)],
                            buf.at[pl.ds(pl.multiple_of(slot * tiles, tiles), n * tiles)],
                            sems.at[b],
                        ).start()

                return carry

            total, _ = incoming(counts_ref, member_ref[0], n_dev, n_member, visit, 0)
            filled[0] = (total - member_ref[0] + n_member - 1) >> 3

        def drain(i, carry):
            pltpu.make_async_copy(got_ref.at[pl.ds(0, tiles)], buf.at[pl.ds(0, tiles)], sems.at[g]).wait()
            return carry

        lax.fori_loop(0, pending[g], drain, 0)
        index = g * STEP + lax.broadcasted_iota(jnp.int32, (8, LANES), 0)
        for r in range(STEP // 8):
            real = index + r * 8 < filled[0]
            for k in range(tiles):
                at = (g * STEP + r * 8) * tiles + k
                rows = buf[pl.ds(at, 8, stride=tiles), :]
                out_ref[r * 8 : r * 8 + 8, k * LANES : (k + 1) * LANES] = jnp.where(real, rows, 0)

    return pl.pallas_call(
        kernel,
        grid=(steps,),
        in_specs=[smem_spec(), smem_spec(), any_spec()],
        out_specs=pl.BlockSpec((STEP, width), lambda g: (g, 0)),
        out_shape=jax.ShapeDtypeStruct((capacity, width), got.dtype),
        scratch_shapes=[
            pltpu.VMEM((capacity * tiles, LANES), got.dtype),
            pltpu.SMEM((steps,), jnp.int32),
            pltpu.SMEM((1,), jnp.int32),
            pltpu.SemaphoreType.DMA((steps,)),
        ],
        name="unpack_rows",
    )(counts, member, got)


NEAR = 112
EDGES = (0, 56, 144, 216)
OWN = 128
PLACES = 2 * (NEAR + EDGES[-1]) + OWN


def segments(hop):
    return [(EDGES[j], EDGES[j + 1] - EDGES[j]) for j in range(min(3, 5 - hop))]


def pack_relay(source, tokens, offset, sizes):
    examples, width = tokens.shape
    tiles = width // LANES
    tiled = tokens.reshape(examples // 8, 8, tiles, LANES).transpose(0, 2, 1, 3)[..., None, :]
    parts = 4

    def kernel(source_ref, tok_ref, *rest):
        outs, (buf, sem_in, sem_out) = rest[: len(sizes)], rest[len(sizes) :]
        each = examples // 8 // parts
        loads = [
            pltpu.make_async_copy(tok_ref.at[pl.ds(i * each, each)], buf.at[pl.ds(i * each, each)], sem_in)
            for i in range(parts)
        ]
        for load in loads:
            load.start()
        for load in loads:
            load.wait()
        start = offset
        for out, size in zip(outs, sizes):

            def some(i, carry, out=out, start=start):
                for j in range(8):
                    row = source_ref[start + i * 8 + j]
                    pltpu.make_async_copy(slot_of(buf, row), out.at[i * 8 + j], sem_out).start()
                return carry

            lax.fori_loop(0, size // 8, some, 0)
            start += size
        for out in outs:
            pltpu.make_async_copy(out, out, sem_out).wait()

    packed = pl.pallas_call(
        kernel,
        in_specs=[smem_spec(), any_spec()],
        out_specs=[any_spec()] * len(sizes),
        out_shape=[jax.ShapeDtypeStruct((n, tiles, 1, LANES), tokens.dtype) for n in sizes],
        scratch_shapes=[
            pltpu.VMEM((examples // 8, tiles, 8, 1, LANES), tokens.dtype),
            pltpu.SemaphoreType.DMA,
            pltpu.SemaphoreType.DMA,
        ],
    )(source, tiled)
    return [rows.reshape(-1, LANES) for rows in packed]


ROUNDS = ((0, 1), (2,), (3, 4))


def lanes_of(hop):
    if hop == 0:
        return [((0,), 4)]
    if hop == 4:
        return [((0, 1), 4)]
    return [((0,), 4), ((1,), 4)]


def slot_map():
    found = {}
    for n, hops in enumerate(ROUNDS):
        skip = 0
        for hop in hops:
            for sides, slots in lanes_of(hop):
                for side in sides:
                    found[hop if side == 0 else (8 - hop) % 8] = (n, skip)
                skip += slots
        for d, (m, at) in list(found.items()):
            if m == n and not isinstance(at, tuple):
                found[d] = (m, (at, skip))
    return {d: (n, rows, at) for d, (n, (at, rows)) in found.items()}


def spread(n, place, counts, befores, pieces, n_member, tiles, onto=None):
    slots = slot_map()
    width = next(rows for m, rows, _ in slots.values() if m == n)
    total = 4 * n_member * width * tiles
    origins, held = {}, 0
    for hop, side, start, rows, _ in pieces:
        if (hop, side) not in origins:
            rows_in = (OWN, NEAR, EDGES[3], EDGES[2], EDGES[1])[hop]
            origins[hop, side] = (held, rows_in)
            held += rows_in + 32
    arrays = [array for *_, array in pieces]
    laid = sum(4 * (16 if hop == 4 else 32) for hop, _ in origins)
    base_of = [] if onto is None else [onto]

    def kernel(place_ref, counts_ref, befores_ref, *rest):
        rest = rest[len(base_of) :]
        ins, (out, buf, sem_in, sem_out) = rest[: len(pieces)], rest[len(pieces) :]
        loads = []
        for (hop, side, start, rows, _), ref in zip(pieces, ins):
            at = (origins[hop, side][0] + start) * tiles
            loads.append(pltpu.make_async_copy(ref, buf.at[pl.ds(at, rows * tiles)], sem_in))
        for load in loads:
            load.start()
        z = place_ref[0]
        todo = []
        for (hop, side), (base, rows_in) in origins.items():
            sign = 1 - 2 * side
            origin = (z - sign * hop) & 7

            def share(y, k, origin=origin, sign=sign, side=side):
                count = counts_ref[origin * 32 + y * 8 + ((origin + sign * k) & 7)]
                return (count + 1 - side) >> 1 if k == 4 else count

            at = 0
            if hop > 1:
                for k in range(hop + 1, 5):
                    for y in range(4):
                        at += share(y, k)
            for y in range(4):
                todo.append((hop, side, y, base + jnp.minimum(at, rows_in), befores_ref[origin * 32 + y * 8 + z]))
                at += share(y, hop)
        for load in loads:
            load.wait()
        for hop, side, y, first, before in todo:
            skip = slots[hop if side == 0 else (8 - hop) % 8][2]
            for j in range(16 if hop == 4 else 32):
                local = 2 * j + side if hop == 4 else j
                member = (before + local) & (n_member - 1)
                to = (y * n_member + member) * width + skip + local // n_member
                pltpu.make_async_copy(
                    buf.at[pl.ds(pl.multiple_of((first + j) * tiles, tiles), tiles)],
                    out.at[pl.ds(pl.multiple_of(to * tiles, tiles), tiles)],
                    sem_out,
                ).start()
        whole = out.at[pl.ds(0, laid * tiles)]
        pltpu.make_async_copy(whole, whole, sem_out).wait()

    return pl.pallas_call(
        kernel,
        in_specs=[smem_spec()] * 3 + [any_spec()] * (len(base_of) + len(pieces)),
        out_specs=any_spec(),
        out_shape=jax.ShapeDtypeStruct((total, LANES), arrays[0].dtype),
        input_output_aliases={3: 0} if base_of else {},
        scratch_shapes=[
            pltpu.VMEM((held * tiles, LANES), arrays[0].dtype),
            pltpu.SemaphoreType.DMA,
            pltpu.SemaphoreType.DMA,
        ],
    )(place, counts, befores, *base_of, *arrays)


def copy_senders(d, slots_of, place_ref, counts_ref, befores_ref, n_member, start):
    _, rows_each, skip = slots_of[d]
    member = place_ref[1]
    origin = (place_ref[0] - d) & 7

    def sender(i, total):
        s = ((i >> 3) * 8 + origin) * n_member + (i & 7)
        before = befores_ref[s]
        first = (member - before) & (n_member - 1)
        rows = (counts_ref[s] - first + n_member - 1) >> 3
        slot = (before + first) >> 3
        for q in range(4):

            @pl.when(q < rows)
            def _(q=q):
                start(i * rows_each + skip + q, slot + q)

        return total + rows

    return lax.fori_loop(0, 4 * n_member, sender, 0)


def slot_of(ref, slot):
    return ref.at[slot >> 3, :, slot & 7]


def unpack_early(place, counts, befores, got, n_member, capacity, tiles):
    slots_of = slot_map()
    groups = capacity // 8

    def kernel(place_ref, counts_ref, befores_ref, *rest):
        ins, (out_ref, buf, zero, sem_in, sem_out) = rest[: len(got)], rest[len(got) :]
        zero[...] = jnp.zeros(zero.shape, zero.dtype)
        moved = 0
        for d in range(8):
            n = slots_of[d][0]
            if n < len(got):

                def start(row, slot, n=n):
                    pltpu.make_async_copy(ins[n].at[row], slot_of(buf, slot), sem_in).start()

                moved += copy_senders(d, slots_of, place_ref, counts_ref, befores_ref, n_member, start)

        def drain(i, carry):
            pltpu.make_async_copy(ins[0].at[0], buf.at[0, :, 0], sem_in).wait()
            return carry

        lax.fori_loop(0, moved, drain, 0)
        end = 32 * n_member - 1
        filled = (befores_ref[end] + counts_ref[end] - place_ref[1] + n_member - 1) >> 3
        whole, extra = filled >> 3, filled & 7

        def group(g, carry):
            @pl.when(g < whole)
            def _():
                pltpu.make_async_copy(buf.at[g], out_ref.at[g], sem_out).start()

            @pl.when((g > whole) | ((g == whole) & (extra == 0)))
            def _():
                pltpu.make_async_copy(zero, out_ref.at[g], sem_out).start()

            @pl.when((g == whole) & (extra > 0))
            def _():
                for k in range(8):

                    @pl.when(k < extra)
                    def _(k=k):
                        pltpu.make_async_copy(buf.at[g, :, k], out_ref.at[g, :, k], sem_out).start()

                    @pl.when(k >= extra)
                    def _(k=k):
                        pltpu.make_async_copy(zero.at[:, k], out_ref.at[g, :, k], sem_out).start()

            return carry

        lax.fori_loop(0, groups, group, 0)
        pltpu.make_async_copy(buf, out_ref, sem_out).wait()

    return pl.pallas_call(
        kernel,
        in_specs=[smem_spec()] * 3 + [any_spec()] * len(got),
        out_specs=any_spec(),
        out_shape=jax.ShapeDtypeStruct((groups, tiles, 8, 1, LANES), got[0].dtype),
        scratch_shapes=[
            pltpu.VMEM((groups, tiles, 8, 1, LANES), got[0].dtype),
            pltpu.VMEM((tiles, 8, 1, LANES), got[0].dtype),
            pltpu.SemaphoreType.DMA,
            pltpu.SemaphoreType.DMA,
        ],
        name="unpack_early",
    )(place, counts, befores, *got)


def unpack_last(place, counts, befores, early, last, n_member):
    slots_of = slot_map()
    late = [d for d in range(8) if slots_of[d][0] == len(ROUNDS) - 1]
    last = pltpu.with_memory_space_constraint(last, pltpu.MemorySpace.VMEM)

    def kernel(place_ref, counts_ref, befores_ref, early_ref, buf, out_ref, sem_out):

        def start(row, slot):
            pltpu.make_async_copy(buf.at[row], slot_of(out_ref, slot), sem_out).start()

        moved = 0
        for d in late:
            moved += copy_senders(d, slots_of, place_ref, counts_ref, befores_ref, n_member, start)

        def drain(i, carry):
            pltpu.make_async_copy(buf.at[0], out_ref.at[0, :, 0], sem_out).wait()
            return carry

        lax.fori_loop(0, moved, drain, 0)

    return pl.pallas_call(
        kernel,
        in_specs=[smem_spec()] * 3 + [any_spec(), pl.BlockSpec(memory_space=pltpu.MemorySpace.VMEM)],
        out_specs=any_spec(),
        out_shape=jax.ShapeDtypeStruct(early.shape, early.dtype),
        input_output_aliases={3: 0},
        scratch_shapes=[pltpu.SemaphoreType.DMA],
        name="unpack_last",
    )(place, counts, befores, early, last)


def relay_source(counts, local_rank, onehot, z):
    owner = jnp.arange(32, dtype=jnp.int32)
    y, d = owner // 8, (owner - z) % 8
    dist = jnp.minimum(d, 8 - d)
    earlier = (((4 - dist) * 4 + y)[None, :] < ((4 - dist) * 4 + y)[:, None]) & ((dist > 1)[None, :] == (dist > 1)[:, None])

    def start(members, sizes):
        return jnp.sum(jnp.where(earlier & members[None, :], sizes[None, :], 0), axis=1)

    ahead, back = (d >= 1) & (d <= 4), d >= 4
    start_ahead = start(ahead, jnp.where(d == 4, (counts + 1) >> 1, counts))
    start_back = start(back, jnp.where(d == 4, counts >> 1, counts))
    far_ahead, far_back, mine = 2 * NEAR, 2 * NEAR + EDGES[-1], 2 * NEAR + 2 * EDGES[-1]
    first = jnp.where(d == 0, mine, jnp.where(ahead, jnp.where(d == 1, 0, far_ahead), jnp.where(d == 7, NEAR, far_back)))
    base = first + jnp.where(d == 0, start(d == 0, counts), jnp.where(ahead, start_ahead, start_back))
    other = far_back + start_back
    limit = first + jnp.where(d == 0, OWN, jnp.where(dist == 1, NEAR, EDGES[-1]))

    def pick(values):
        return jnp.sum(onehot * values[None, :], axis=1)

    four = pick((d == 4).astype(jnp.int32)) == 1
    odd = four & ((local_rank & 1) == 1)
    position = jnp.where(odd, pick(other), pick(base)) + jnp.where(four, local_rank >> 1, local_rank)
    bound = jnp.where(odd, mine, pick(limit))
    position = jnp.where((jnp.sum(onehot, axis=1) == 1) & (position < bound), position, -1)
    example = jnp.arange(onehot.shape[0], dtype=jnp.int32)
    places = jnp.arange(PLACES, dtype=jnp.int32)
    return jnp.sum(jnp.where(position[None, :] == places[:, None], example[None, :], 0), axis=1)


def by_owner(values, position, size):
    places = jnp.arange(size, dtype=jnp.int32)
    return jnp.sum(jnp.where(position[None, :] == places[:, None], values[None, :], 0), axis=1)


def relay_fits(table):
    n_dev = table.shape[0]
    z = (jnp.arange(n_dev, dtype=jnp.int32)[:, None] // 8) % 8
    d = (jnp.arange(32, dtype=jnp.int32)[None, :] - z) % 8
    plus = jnp.where(d == 4, (table + 1) >> 1, table)
    minus = jnp.where(d == 4, table >> 1, table)
    over = jnp.zeros((), jnp.int32)
    for least, most, cap in ((1, 1, NEAR), (2, 4, EDGES[3]), (3, 4, EDGES[2]), (4, 4, EDGES[1])):
        ahead = jnp.sum(jnp.where((d >= least) & (d <= most), plus, 0), axis=1)
        back = jnp.sum(jnp.where((d <= 8 - least) & (d >= 8 - most), minus, 0), axis=1)
        over = jnp.maximum(over, jnp.max(jnp.maximum(ahead, back)) - cap)
    return over <= 0


def exchange(value, axes=DP_GROUP):
    return lax.all_to_all(value, axes, split_axis=0, concat_axis=0, tiled=True)


def hop_on(value, step, axis="dp_1"):
    count = lax.axis_size(axis)
    return lax.ppermute(value, axis, [(i, (i + step) % count) for i in range(count)])


DOUBLING = (
    ("group_1", 1), ("group_0", 1), ("group_0", 2), ("dp_0", 1), ("dp_0", 2), ("dp_1", 1), ("dp_1", 2), ("dp_1", 4),
)


def program(keys, cut, owner, tokens):
    examples = keys.shape[0]
    width = tokens.shape[1]
    tiles = width // LANES
    n_owner = lax.axis_size(DP)
    n_member = lax.axis_size(GROUP)
    n_dev = n_owner * n_member
    slots = 2 * examples // n_dev
    capacity = 2 * examples
    most = slots * n_member
    me = lax.axis_index(DP_GROUP)
    member = lax.axis_index(GROUP)
    y, z = lax.axis_index("dp_0"), lax.axis_index("dp_1")
    bins_of = keys >> KEY_SHIFT
    dest = owner[:, 0]
    kept = bins_of >= cut[0]
    owners = jnp.arange(n_owner, dtype=jnp.int32)
    onehot = ((dest[:, None] == owners[None, :]) & kept[:, None]).astype(jnp.int32)
    counts = jnp.sum(onehot, axis=0)
    index = jnp.arange(examples, dtype=jnp.int32)
    lower = (index[None, :] < index[:, None]).astype(jnp.bfloat16)
    running = jnp.dot(lower, onehot.astype(jnp.bfloat16), preferred_element_type=jnp.float32).astype(jnp.int32)
    local_rank = jnp.sum(running * onehot, axis=1)
    source = relay_source(counts, local_rank, onehot, z)
    near = pack_relay(source, tokens, 0, [NEAR] * 2)
    *far, own = pack_relay(source, tokens, 2 * NEAR, [n for _, n in segments(1)] * 2 + [OWN])
    plus, minus = far[:3], far[3:]

    hist = jnp.zeros((BINS,), jnp.int32).at[bins_of].add(1)
    for axis, step in DOUBLING:
        hist = hist + hop_on(hist, step, axis)
    own_keys = by_owner(keys, jnp.where(kept, dest * most + local_rank, -1), n_owner * most).reshape(n_owner, 1, most)
    own_keys = jnp.broadcast_to(own_keys, (n_owner, n_member, most)).reshape(n_dev, most)
    first = jnp.concatenate([jnp.broadcast_to(counts[None, :], (n_dev, n_owner)), own_keys], axis=1)
    first, _ = lax.optimization_barrier((first, source))
    first = exchange(first)
    table = first[:, :n_owner]
    got_keys = first[:, n_owner:].reshape(-1)
    device = jnp.arange(n_dev, dtype=jnp.int32)
    below = (device[None, :] < device[:, None]).astype(jnp.bfloat16)
    befores = jnp.dot(below, table.astype(jnp.bfloat16), preferred_element_type=jnp.float32).astype(jnp.int32)
    before = lax.dynamic_slice_in_dim(befores, me, 1, axis=0)[0]

    def column(values):
        return lax.dynamic_slice_in_dim(values, me // n_member, 1, axis=1)[:, 0]

    def line(values):
        return lax.dynamic_slice(values.reshape(4, 8, n_member, n_owner), (y, 0, member, 0), (1, 8, 1, n_owner)).reshape(-1)

    mine, mine_before = column(table), column(befores)
    line_counts, line_befores = line(table), line(befores)
    fits = relay_fits(table)
    place = jnp.stack([z, member]).astype(jnp.int32)

    slot_bins = place_bins(mine, member[None], got_keys, n_dev, n_member, slots, capacity)

    arrived = {0: [(0, 0, 0, OWN, own)]}
    near = [hop_on(near[0], 1), hop_on(near[1], -1)]
    arrived[1] = [(1, i, 0, NEAR, v) for i, v in enumerate(near)]
    for k in range(1, 5):
        spans = segments(k)
        plus = [hop_on(v, 1) for v in plus[: len(spans)]]
        minus = [hop_on(v, -1) for v in minus[: len(spans)]]
        if k > 1:
            arrived[k] = [(k, i, *span, v) for i, side in enumerate((plus, minus)) for span, v in zip(spans, side)]
    got = []
    for n, hops in enumerate(ROUNDS):
        calls = [[k] for k in hops] if hops[-1] == 4 else [hops]
        laid = None
        for ks in calls:
            laid = spread(n, place, line_counts, line_befores, [p for k in ks for p in arrived[k]], n_member, tiles, laid)
        laid = laid.reshape(n_owner, -1, tiles, LANES)
        if n > 0:
            laid, got[-1] = lax.optimization_barrier((laid, got[-1]))
        got.append(exchange(laid, ("dp_0",) + GROUP).reshape(-1, tiles, 1, LANES))

    early = unpack_early(place, mine, mine_before, got[:-1], n_member, capacity, tiles)
    packed = unpack_last(place, mine, mine_before, early, got[-1], n_member)
    packed = packed.reshape(capacity // 8, tiles, 8, LANES).transpose(0, 2, 1, 3).reshape(capacity, width)

    def direct(state):
        info = jnp.concatenate([cut, before])
        send_rows, _ = pack_rows(keys, dest, info, tokens, n_dev, n_member, slots)
        rows = exchange(send_rows.reshape(n_dev, slots, tiles, LANES)).reshape(-1, LANES)
        return jnp.ones((), jnp.bool_), unpack_rows(mine, member[None], rows, n_dev, n_member, slots, capacity, width)

    _, packed = lax.while_loop(lambda state: ~state[0], direct, (fits, packed))

    suffix = jnp.cumsum(hist.astype(jnp.float32)[::-1])[::-1]
    total = jnp.maximum(suffix[cut[0]], 1.0)
    weights = jnp.where(slot_bins >= 0, suffix[jnp.maximum(slot_bins, 0)] / total, 0.0)
    return (hist, packed, weights)


def solution(mesh):
    torus = Mesh(mesh.devices.reshape(4, 8, 4, 2), ("dp_0", "dp_1", "group_0", "group_1"))
    placed = (P(DP_GROUP), P(), P(DP_GROUP, None), P(DP_GROUP, None))
    return jax.shard_map(
        program,
        mesh=torus,
        in_specs=placed,
        out_specs=(P(), P(DP_GROUP, None), P(DP_GROUP)),
        check_vma=False,
    )
```

```python
import jax
import jax.numpy as jnp
from jax import lax
from jax.experimental import pallas as pl
from jax.experimental.pallas import tpu as pltpu
from jax.sharding import Mesh
from jax.sharding import PartitionSpec as P


BINS = 4096
KEY_SHIFT = 18
DP = ("dp_0", "dp_1")
GROUP = ("group_0", "group_1")
DP_GROUP = ("dp_0", "dp_1", "group_0", "group_1")
LANES = 128
STEP = 64

SMEM = pltpu.MemorySpace.SMEM
VMEM = pltpu.MemorySpace.VMEM


def smem_spec():
    return pl.BlockSpec(memory_space=SMEM)


def any_spec():
    return pl.BlockSpec(memory_space=pltpu.MemorySpace.HBM)


def pack_rows(keys, dest, info, tokens, n_dev, n_member, slots):
    examples, width = tokens.shape
    tiles = width // LANES
    steps = examples // STEP
    n_owner = n_dev // n_member

    def kernel(keys_ref, dest_ref, info_ref, tok_ref, rows_ref, meta_ref, buf, seen, sent, sem):
        g = pl.program_id(0)

        @pl.when(g == 0)
        def _():
            sent[0] = 0
            for o in range(n_owner):
                seen[o] = 0

        @pl.when(g < steps)
        def _():
            for r in range(STEP // 8):
                for k in range(tiles):
                    at = (g * STEP + r * 8) * tiles + k
                    buf[pl.ds(at, 8, stride=tiles), :] = tok_ref[r * 8 : r * 8 + 8, k * LANES : (k + 1) * LANES]

        @pl.when(g > 0)
        def _():
            lowest = info_ref[0] << KEY_SHIFT

            def row(i, total):
                key = keys_ref[i]
                kept = key >= lowest

                @pl.when(kept)
                def _():
                    o = dest_ref[i]
                    local = seen[o]
                    seen[o] = local + 1
                    member = (info_ref[1 + o] + local) & (n_member - 1)
                    to = (o * n_member + member) * slots + local // n_member
                    meta_ref[to] = key
                    pltpu.make_async_copy(
                        buf.at[pl.ds(pl.multiple_of(i * tiles, tiles), tiles)],
                        rows_ref.at[pl.ds(pl.multiple_of(to * tiles, tiles), tiles)],
                        sem,
                    ).start()

                return total + kept.astype(jnp.int32)

            start = (g - 1) * STEP
            sent[0] = lax.fori_loop(start, start + STEP, row, sent[0])

        @pl.when(g == steps)
        def _():
            def drain(i, carry):
                pltpu.make_async_copy(buf.at[pl.ds(0, tiles)], rows_ref.at[pl.ds(0, tiles)], sem).wait()
                return carry

            lax.fori_loop(0, sent[0], drain, 0)

    return pl.pallas_call(
        kernel,
        grid=(steps + 1,),
        in_specs=[
            smem_spec(),
            smem_spec(),
            smem_spec(),
            pl.BlockSpec((STEP, width), lambda g: (jnp.minimum(g, steps - 1), 0)),
        ],
        out_specs=[any_spec(), smem_spec()],
        out_shape=[
            jax.ShapeDtypeStruct((n_dev * slots * tiles, LANES), tokens.dtype),
            jax.ShapeDtypeStruct((n_dev * slots,), keys.dtype),
        ],
        scratch_shapes=[
            pltpu.VMEM((examples * tiles, LANES), tokens.dtype),
            pltpu.SMEM((n_owner,), jnp.int32),
            pltpu.SMEM((1,), jnp.int32),
            pltpu.SemaphoreType.DMA,
        ],
        name="pack_rows",
    )(keys, dest, info, tokens)


def incoming(counts_ref, member, n_dev, n_member, visit, carry):
    def source(s, state):
        before, carry = state
        count = counts_ref[s]
        first = (member - before) & (n_member - 1)
        rows = (count - first + n_member - 1) >> 3
        carry = visit(s, (before + first) >> 3, rows, carry)
        return before + count, carry

    return lax.fori_loop(0, n_dev, source, (0, carry))


def place_bins(counts, member, got_keys, n_dev, n_member, slots, capacity):
    def kernel(counts_ref, member_ref, keys_ref, out_ref):
        def clear(i, carry):
            for j in range(8):
                out_ref[i * 8 + j] = -1
            return carry

        lax.fori_loop(0, capacity // 8, clear, 0)

        def visit(s, slot, rows, carry):
            at = s * (slots * n_member) + ((member_ref[0] - carry) & (n_member - 1))

            def one(q, c):
                out_ref[slot + q] = keys_ref[at + q * n_member] >> KEY_SHIFT
                return c

            lax.fori_loop(0, rows, one, 0)
            return carry + counts_ref[s]

        incoming(counts_ref, member_ref[0], n_dev, n_member, visit, 0)

    return pl.pallas_call(
        kernel,
        in_specs=[smem_spec()] * 3,
        out_specs=smem_spec(),
        out_shape=jax.ShapeDtypeStruct((capacity,), jnp.int32),
        name="place_bins",
    )(counts, member, got_keys)


def unpack_rows(counts, member, got, n_dev, n_member, slots, capacity, width):
    tiles = width // LANES
    steps = capacity // STEP

    def kernel(counts_ref, member_ref, got_ref, out_ref, buf, pending, filled, sems):
        g = pl.program_id(0)

        @pl.when(g == 0)
        def _():
            for b in range(steps):
                pending[b] = 0

            def visit(s, slot, rows, carry):
                b = slot // STEP

                @pl.when(rows > 0)
                def _():
                    pending[b] = pending[b] + rows

                for n in range(1, slots + 1):

                    @pl.when(rows == n)
                    def _(n=n):
                        pltpu.make_async_copy(
                            got_ref.at[pl.ds(pl.multiple_of(s * (slots * tiles), tiles), n * tiles)],
                            buf.at[pl.ds(pl.multiple_of(slot * tiles, tiles), n * tiles)],
                            sems.at[b],
                        ).start()

                return carry

            total, _ = incoming(counts_ref, member_ref[0], n_dev, n_member, visit, 0)
            filled[0] = (total - member_ref[0] + n_member - 1) >> 3

        def drain(i, carry):
            pltpu.make_async_copy(got_ref.at[pl.ds(0, tiles)], buf.at[pl.ds(0, tiles)], sems.at[g]).wait()
            return carry

        lax.fori_loop(0, pending[g], drain, 0)
        index = g * STEP + lax.broadcasted_iota(jnp.int32, (8, LANES), 0)
        for r in range(STEP // 8):
            real = index + r * 8 < filled[0]
            for k in range(tiles):
                at = (g * STEP + r * 8) * tiles + k
                rows = buf[pl.ds(at, 8, stride=tiles), :]
                out_ref[r * 8 : r * 8 + 8, k * LANES : (k + 1) * LANES] = jnp.where(real, rows, 0)

    return pl.pallas_call(
        kernel,
        grid=(steps,),
        in_specs=[smem_spec(), smem_spec(), any_spec()],
        out_specs=pl.BlockSpec((STEP, width), lambda g: (g, 0)),
        out_shape=jax.ShapeDtypeStruct((capacity, width), got.dtype),
        scratch_shapes=[
            pltpu.VMEM((capacity * tiles, LANES), got.dtype),
            pltpu.SMEM((steps,), jnp.int32),
            pltpu.SMEM((1,), jnp.int32),
            pltpu.SemaphoreType.DMA((steps,)),
        ],
        name="unpack_rows",
    )(counts, member, got)


NEAR = 112
EDGES = (0, 56, 144, 216)
OWN = 128
PLACES = 2 * (NEAR + EDGES[-1]) + OWN


def segments(hop):
    return [(EDGES[j], EDGES[j + 1] - EDGES[j]) for j in range(min(3, 5 - hop))]


def pack_relay(source, tokens, offset, sizes):
    examples, width = tokens.shape
    tiles = width // LANES
    tiled = tokens.reshape(examples // 8, 8, tiles, LANES).transpose(0, 2, 1, 3)[..., None, :]
    parts = 4

    def kernel(source_ref, tok_ref, *rest):
        outs, (buf, sem_in, sem_out) = rest[: len(sizes)], rest[len(sizes) :]
        each = examples // 8 // parts
        loads = [
            pltpu.make_async_copy(tok_ref.at[pl.ds(i * each, each)], buf.at[pl.ds(i * each, each)], sem_in)
            for i in range(parts)
        ]
        for load in loads:
            load.start()
        for load in loads:
            load.wait()
        start = offset
        for out, size in zip(outs, sizes):

            def some(i, carry, out=out, start=start):
                for j in range(8):
                    row = source_ref[0, start + i * 8 + j]
                    pltpu.make_async_copy(slot_of(buf, row), out.at[i * 8 + j], sem_out).start()
                return carry

            lax.fori_loop(0, size // 8, some, 0)
            start += size
        for out in outs:
            pltpu.make_async_copy(out, out, sem_out).wait()

    packed = pl.pallas_call(
        kernel,
        in_specs=[smem_spec(), any_spec()],
        out_specs=[any_spec()] * len(sizes),
        out_shape=[jax.ShapeDtypeStruct((n, tiles, 1, LANES), tokens.dtype) for n in sizes],
        scratch_shapes=[
            pltpu.VMEM((examples // 8, tiles, 8, 1, LANES), tokens.dtype),
            pltpu.SemaphoreType.DMA,
            pltpu.SemaphoreType.DMA,
        ],
    )(source, tiled)
    return [rows.reshape(-1, LANES) for rows in packed]


ROUNDS = ((0, 1), (2,), (3, 4))


def lanes_of(hop):
    if hop == 0:
        return [((0,), 4)]
    if hop == 4:
        return [((0, 1), 4)]
    return [((0,), 4), ((1,), 4)]


def slot_map():
    found = {}
    for n, hops in enumerate(ROUNDS):
        skip = 0
        for hop in hops:
            for sides, slots in lanes_of(hop):
                for side in sides:
                    found[hop if side == 0 else (8 - hop) % 8] = (n, skip)
                skip += slots
        for d, (m, at) in list(found.items()):
            if m == n and not isinstance(at, tuple):
                found[d] = (m, (at, skip))
    return {d: (n, rows, at) for d, (n, (at, rows)) in found.items()}


def spread(n, place, counts, befores, pieces, n_member, tiles, onto=None):
    slots = slot_map()
    width = next(rows for m, rows, _ in slots.values() if m == n)
    total = 4 * n_member * width * tiles
    origins, held = {}, 0
    for hop, side, start, rows, _ in pieces:
        if (hop, side) not in origins:
            rows_in = (OWN, NEAR, EDGES[3], EDGES[2], EDGES[1])[hop]
            origins[hop, side] = (held, rows_in)
            held += rows_in + 32
    arrays = [array for *_, array in pieces]
    laid = sum(4 * (16 if hop == 4 else 32) for hop, _ in origins)
    base_of = [] if onto is None else [onto]

    def kernel(place_ref, counts_ref, befores_ref, *rest):
        rest = rest[len(base_of) :]
        ins, (out, buf, sem_in, sem_out) = rest[: len(pieces)], rest[len(pieces) :]
        loads = []
        for (hop, side, start, rows, _), ref in zip(pieces, ins):
            at = (origins[hop, side][0] + start) * tiles
            loads.append(pltpu.make_async_copy(ref, buf.at[pl.ds(at, rows * tiles)], sem_in))
        for load in loads:
            load.start()
        z = place_ref[0]
        todo = []
        for (hop, side), (base, rows_in) in origins.items():
            sign = 1 - 2 * side
            origin = (z - sign * hop) & 7

            def share(y, k, origin=origin, sign=sign, side=side):
                count = counts_ref[origin * 32 + y * 8 + ((origin + sign * k) & 7)]
                return (count + 1 - side) >> 1 if k == 4 else count

            at = 0
            if hop > 1:
                for k in range(hop + 1, 5):
                    for y in range(4):
                        at += share(y, k)
            for y in range(4):
                todo.append((hop, side, y, base + jnp.minimum(at, rows_in), befores_ref[origin * 32 + y * 8 + z]))
                at += share(y, hop)
        for load in loads:
            load.wait()
        for hop, side, y, first, before in todo:
            skip = slots[hop if side == 0 else (8 - hop) % 8][2]
            for j in range(16 if hop == 4 else 32):
                local = 2 * j + side if hop == 4 else j
                member = (before + local) & (n_member - 1)
                to = (y * n_member + member) * width + skip + local // n_member
                pltpu.make_async_copy(
                    buf.at[pl.ds(pl.multiple_of((first + j) * tiles, tiles), tiles)],
                    out.at[pl.ds(pl.multiple_of(to * tiles, tiles), tiles)],
                    sem_out,
                ).start()
        whole = out.at[pl.ds(0, laid * tiles)]
        pltpu.make_async_copy(whole, whole, sem_out).wait()

    return pl.pallas_call(
        kernel,
        in_specs=[smem_spec()] * 3 + [any_spec()] * (len(base_of) + len(pieces)),
        out_specs=any_spec(),
        out_shape=jax.ShapeDtypeStruct((total, LANES), arrays[0].dtype),
        input_output_aliases={3: 0} if base_of else {},
        scratch_shapes=[
            pltpu.VMEM((held * tiles, LANES), arrays[0].dtype),
            pltpu.SemaphoreType.DMA,
            pltpu.SemaphoreType.DMA,
        ],
    )(place, counts, befores, *base_of, *arrays)


def copy_senders(d, slots_of, place_ref, counts_ref, befores_ref, n_member, start):
    _, rows_each, skip = slots_of[d]
    member = place_ref[1]
    origin = (place_ref[0] - d) & 7

    def sender(i, total):
        s = ((i >> 3) * 8 + origin) * n_member + (i & 7)
        before = befores_ref[s]
        first = (member - before) & (n_member - 1)
        rows = (counts_ref[s] - first + n_member - 1) >> 3
        slot = (before + first) >> 3
        for q in range(4):

            @pl.when(q < rows)
            def _(q=q):
                start(i * rows_each + skip + q, slot + q)

        return total + rows

    return lax.fori_loop(0, 4 * n_member, sender, 0)


def slot_of(ref, slot):
    return ref.at[slot >> 3, :, slot & 7]


def unpack_early(place, counts, befores, got, n_member, capacity, tiles):
    slots_of = slot_map()
    groups = capacity // 8

    def kernel(place_ref, counts_ref, befores_ref, *rest):
        ins, (out_ref, buf, zero, sem_in, sem_out) = rest[: len(got)], rest[len(got) :]
        zero[...] = jnp.zeros(zero.shape, zero.dtype)
        moved = 0
        for d in range(8):
            n = slots_of[d][0]
            if n < len(got):

                def start(row, slot, n=n):
                    pltpu.make_async_copy(ins[n].at[row], slot_of(buf, slot), sem_in).start()

                moved += copy_senders(d, slots_of, place_ref, counts_ref, befores_ref, n_member, start)

        def drain(i, carry):
            pltpu.make_async_copy(ins[0].at[0], buf.at[0, :, 0], sem_in).wait()
            return carry

        lax.fori_loop(0, moved, drain, 0)
        end = 32 * n_member - 1
        filled = (befores_ref[end] + counts_ref[end] - place_ref[1] + n_member - 1) >> 3
        whole, extra = filled >> 3, filled & 7

        def group(g, carry):
            @pl.when(g < whole)
            def _():
                pltpu.make_async_copy(buf.at[g], out_ref.at[g], sem_out).start()

            @pl.when((g > whole) | ((g == whole) & (extra == 0)))
            def _():
                pltpu.make_async_copy(zero, out_ref.at[g], sem_out).start()

            @pl.when((g == whole) & (extra > 0))
            def _():
                for k in range(8):

                    @pl.when(k < extra)
                    def _(k=k):
                        pltpu.make_async_copy(buf.at[g, :, k], out_ref.at[g, :, k], sem_out).start()

                    @pl.when(k >= extra)
                    def _(k=k):
                        pltpu.make_async_copy(zero.at[:, k], out_ref.at[g, :, k], sem_out).start()

            return carry

        lax.fori_loop(0, groups, group, 0)
        pltpu.make_async_copy(buf, out_ref, sem_out).wait()

    return pl.pallas_call(
        kernel,
        in_specs=[smem_spec()] * 3 + [any_spec()] * len(got),
        out_specs=any_spec(),
        out_shape=jax.ShapeDtypeStruct((groups, tiles, 8, 1, LANES), got[0].dtype),
        scratch_shapes=[
            pltpu.VMEM((groups, tiles, 8, 1, LANES), got[0].dtype),
            pltpu.VMEM((tiles, 8, 1, LANES), got[0].dtype),
            pltpu.SemaphoreType.DMA,
            pltpu.SemaphoreType.DMA,
        ],
        name="unpack_early",
    )(place, counts, befores, *got)


def unpack_last(place, counts, befores, early, last, n_member):
    slots_of = slot_map()
    late = [d for d in range(8) if slots_of[d][0] == len(ROUNDS) - 1]
    last = pltpu.with_memory_space_constraint(last, pltpu.MemorySpace.VMEM)

    def kernel(place_ref, counts_ref, befores_ref, early_ref, buf, out_ref, sem_out):

        def start(row, slot):
            pltpu.make_async_copy(buf.at[row], slot_of(out_ref, slot), sem_out).start()

        moved = 0
        for d in late:
            moved += copy_senders(d, slots_of, place_ref, counts_ref, befores_ref, n_member, start)

        def drain(i, carry):
            pltpu.make_async_copy(buf.at[0], out_ref.at[0, :, 0], sem_out).wait()
            return carry

        lax.fori_loop(0, moved, drain, 0)

    return pl.pallas_call(
        kernel,
        in_specs=[smem_spec()] * 3 + [any_spec(), pl.BlockSpec(memory_space=pltpu.MemorySpace.VMEM)],
        out_specs=any_spec(),
        out_shape=jax.ShapeDtypeStruct(early.shape, early.dtype),
        input_output_aliases={3: 0},
        scratch_shapes=[pltpu.SemaphoreType.DMA],
        name="unpack_last",
    )(place, counts, befores, early, last)


def plan_relay(keys, dest, cut, z):
    examples = keys.shape[1]
    padded = -(-PLACES // LANES) * LANES

    def across(left, right):
        return lax.dot_general(left, right, (((1,), (1,)), ((), ())), preferred_element_type=jnp.float32)

    def kernel(keys_ref, dest_ref, cut_ref, z_ref, plan_ref, rank_ref, counts_ref):
        kept = (keys_ref[...] >> KEY_SHIFT) >= cut_ref[0]
        owner = lax.broadcasted_iota(jnp.int32, (32, examples), 0)
        hot = (dest_ref[...] == owner) & kept
        ones = jnp.where(hot, 1.0, 0.0).astype(jnp.bfloat16)
        row = lax.broadcasted_iota(jnp.int32, (examples, examples), 0)
        col = lax.broadcasted_iota(jnp.int32, (examples, examples), 1)
        before = jnp.where(row < col, 1.0, 0.0).astype(jnp.bfloat16)
        running = jnp.dot(ones, before, preferred_element_type=jnp.float32).astype(jnp.int32)
        counts = across(jnp.ones((8, examples), jnp.bfloat16), ones).astype(jnp.int32)[0:1, :]
        counts_ref[...] = counts
        rank_ref[...] = jnp.sum(jnp.where(hot, running, 0), axis=0, keepdims=True)

        z = z_ref[0]

        def about(axis):
            o = lax.broadcasted_iota(jnp.int32, (32, 32), axis)
            d = ((o & 7) - z) & 7
            dist = jnp.minimum(d, 8 - d)
            far = jnp.where(dist > 1, 1, 0)
            return d, dist, far * 64 + (4 - dist) * 4 + (o >> 3), far

        d, dist, order, far = about(0)
        d_of, _, order_of, far_of = about(1)
        earlier = (order_of < order) & (far_of == far)

        def start(members, sizes):
            return jnp.sum(jnp.where(earlier & members, sizes, 0), axis=1, keepdims=True)

        start_ahead = start((d_of >= 1) & (d_of <= 4), jnp.where(d_of == 4, (counts + 1) >> 1, counts))
        start_back = start(d_of >= 4, jnp.where(d_of == 4, counts >> 1, counts))
        start_own = start(d_of == 0, jnp.broadcast_to(counts, (32, 32)))
        d, dist = d[:, 0:1], dist[:, 0:1]
        ahead = (d >= 1) & (d <= 4)
        far_ahead, far_back, mine = 2 * NEAR, 2 * NEAR + EDGES[-1], 2 * NEAR + 2 * EDGES[-1]
        first = jnp.where(
            d == 0, mine, jnp.where(ahead, jnp.where(d == 1, 0, far_ahead), jnp.where(d == 7, NEAR, far_back))
        )
        base = first + jnp.where(d == 0, start_own, jnp.where(ahead, start_ahead, start_back))
        other = far_back + start_back
        limit = first + jnp.where(d == 0, OWN, jnp.where(dist == 1, NEAR, EDGES[-1]))
        odd = (d == 4) & ((running & 1) == 1)
        position = jnp.where(odd, other, base) + jnp.where(d == 4, running >> 1, running)
        bound = jnp.where(odd, mine, limit)
        position = jnp.sum(jnp.where(hot & (position < bound), position + 1, 0), axis=0, keepdims=True) - 1

        place = lax.broadcasted_iota(jnp.int32, (padded, examples), 0)
        here = jnp.where(place == position, 1.0, 0.0).astype(jnp.bfloat16)
        part = lax.broadcasted_iota(jnp.int32, (8, examples), 0)
        example = lax.broadcasted_iota(jnp.int32, (8, examples), 1)
        parts = jnp.where(part == 0, example >> 4, jnp.where(part == 1, example & 15, 0))
        found = across(parts.astype(jnp.float32).astype(jnp.bfloat16), here).astype(jnp.int32)
        plan_ref[...] = found[0:1, :] * 16 + found[1:2, :]

    whole = pl.BlockSpec(memory_space=VMEM)
    return pl.pallas_call(
        kernel,
        in_specs=[whole, whole, smem_spec(), smem_spec()],
        out_specs=[whole] * 3,
        out_shape=[
            jax.ShapeDtypeStruct((1, padded), jnp.int32),
            jax.ShapeDtypeStruct((1, examples), jnp.int32),
            jax.ShapeDtypeStruct((1, 32), jnp.int32),
        ],
        name="plan_relay",
    )(keys, dest, cut, z)


def by_owner(values, position, size):
    places = jnp.arange(size, dtype=jnp.int32)
    return jnp.sum(jnp.where(position[None, :] == places[:, None], values[None, :], 0), axis=1)


def relay_fits(table):
    n_dev = table.shape[0]
    z = (jnp.arange(n_dev, dtype=jnp.int32)[:, None] // 8) % 8
    d = (jnp.arange(32, dtype=jnp.int32)[None, :] - z) % 8
    plus = jnp.where(d == 4, (table + 1) >> 1, table)
    minus = jnp.where(d == 4, table >> 1, table)
    over = jnp.zeros((), jnp.int32)
    for least, most, cap in ((1, 1, NEAR), (2, 4, EDGES[3]), (3, 4, EDGES[2]), (4, 4, EDGES[1])):
        ahead = jnp.sum(jnp.where((d >= least) & (d <= most), plus, 0), axis=1)
        back = jnp.sum(jnp.where((d <= 8 - least) & (d >= 8 - most), minus, 0), axis=1)
        over = jnp.maximum(over, jnp.max(jnp.maximum(ahead, back)) - cap)
    return over <= 0


def exchange(value, axes=DP_GROUP):
    return lax.all_to_all(value, axes, split_axis=0, concat_axis=0, tiled=True)


def hop_on(value, step, axis="dp_1"):
    count = lax.axis_size(axis)
    return lax.ppermute(value, axis, [(i, (i + step) % count) for i in range(count)])


DOUBLING = (
    ("group_1", 1), ("group_0", 1), ("group_0", 2), ("dp_0", 1), ("dp_0", 2), ("dp_1", 1), ("dp_1", 2), ("dp_1", 4),
)


def program(keys, cut, owner, tokens):
    examples = keys.shape[0]
    width = tokens.shape[1]
    tiles = width // LANES
    n_owner = lax.axis_size(DP)
    n_member = lax.axis_size(GROUP)
    n_dev = n_owner * n_member
    slots = 2 * examples // n_dev
    capacity = 2 * examples
    most = slots * n_member
    me = lax.axis_index(DP_GROUP)
    member = lax.axis_index(GROUP)
    y, z = lax.axis_index("dp_0"), lax.axis_index("dp_1")
    bins_of = keys >> KEY_SHIFT
    dest = owner[:, 0]
    kept = bins_of >= cut[0]
    source, local_rank, counts = plan_relay(keys[None, :], owner.reshape(1, -1), cut, z[None].astype(jnp.int32))
    local_rank, counts = local_rank[0], counts[0]
    near = pack_relay(source, tokens, 0, [NEAR] * 2)
    *far, own = pack_relay(source, tokens, 2 * NEAR, [n for _, n in segments(1)] * 2 + [OWN])
    plus, minus = far[:3], far[3:]

    hist = jnp.zeros((BINS,), jnp.int32).at[bins_of].add(1)
    for axis, step in DOUBLING:
        hist = hist + hop_on(hist, step, axis)
    own_keys = by_owner(keys, jnp.where(kept, dest * most + local_rank, -1), n_owner * most).reshape(n_owner, 1, most)
    own_keys = jnp.broadcast_to(own_keys, (n_owner, n_member, most)).reshape(n_dev, most)
    first = jnp.concatenate([jnp.broadcast_to(counts[None, :], (n_dev, n_owner)), own_keys], axis=1)
    first, _ = lax.optimization_barrier((first, source))
    first = exchange(first)
    table = first[:, :n_owner]
    got_keys = first[:, n_owner:].reshape(-1)
    device = jnp.arange(n_dev, dtype=jnp.int32)
    below = (device[None, :] < device[:, None]).astype(jnp.bfloat16)
    befores = jnp.dot(below, table.astype(jnp.bfloat16), preferred_element_type=jnp.float32).astype(jnp.int32)
    before = lax.dynamic_slice_in_dim(befores, me, 1, axis=0)[0]

    def column(values):
        return lax.dynamic_slice_in_dim(values, me // n_member, 1, axis=1)[:, 0]

    def line(values):
        return lax.dynamic_slice(values.reshape(4, 8, n_member, n_owner), (y, 0, member, 0), (1, 8, 1, n_owner)).reshape(-1)

    mine, mine_before = column(table), column(befores)
    line_counts, line_befores = line(table), line(befores)
    fits = relay_fits(table)
    place = jnp.stack([z, member]).astype(jnp.int32)

    slot_bins = place_bins(mine, member[None], got_keys, n_dev, n_member, slots, capacity)

    arrived = {0: [(0, 0, 0, OWN, own)]}
    near = [hop_on(near[0], 1), hop_on(near[1], -1)]
    arrived[1] = [(1, i, 0, NEAR, v) for i, v in enumerate(near)]
    for k in range(1, 5):
        spans = segments(k)
        plus = [hop_on(v, 1) for v in plus[: len(spans)]]
        minus = [hop_on(v, -1) for v in minus[: len(spans)]]
        if k > 1:
            arrived[k] = [(k, i, *span, v) for i, side in enumerate((plus, minus)) for span, v in zip(spans, side)]
    got = []
    for n, hops in enumerate(ROUNDS):
        calls = [[k] for k in hops] if hops[-1] == 4 else [hops]
        laid = None
        for ks in calls:
            laid = spread(n, place, line_counts, line_befores, [p for k in ks for p in arrived[k]], n_member, tiles, laid)
        laid = laid.reshape(n_owner, -1, tiles, LANES)
        if n > 0:
            laid, got[-1] = lax.optimization_barrier((laid, got[-1]))
        got.append(exchange(laid, ("dp_0",) + GROUP).reshape(-1, tiles, 1, LANES))

    early = unpack_early(place, mine, mine_before, got[:-1], n_member, capacity, tiles)
    packed = unpack_last(place, mine, mine_before, early, got[-1], n_member)
    packed = packed.reshape(capacity // 8, tiles, 8, LANES).transpose(0, 2, 1, 3).reshape(capacity, width)

    def direct(state):
        info = jnp.concatenate([cut, before])
        send_rows, _ = pack_rows(keys, dest, info, tokens, n_dev, n_member, slots)
        rows = exchange(send_rows.reshape(n_dev, slots, tiles, LANES)).reshape(-1, LANES)
        return jnp.ones((), jnp.bool_), unpack_rows(mine, member[None], rows, n_dev, n_member, slots, capacity, width)

    _, packed = lax.while_loop(lambda state: ~state[0], direct, (fits, packed))

    suffix = jnp.cumsum(hist.astype(jnp.float32)[::-1])[::-1]
    total = jnp.maximum(suffix[cut[0]], 1.0)
    weights = jnp.where(slot_bins >= 0, suffix[jnp.maximum(slot_bins, 0)] / total, 0.0)
    return (hist, packed, weights)


def solution(mesh):
    torus = Mesh(mesh.devices.reshape(4, 8, 4, 2), ("dp_0", "dp_1", "group_0", "group_1"))
    placed = (P(DP_GROUP), P(), P(DP_GROUP, None), P(DP_GROUP, None))
    return jax.shard_map(
        program,
        mesh=torus,
        in_specs=placed,
        out_specs=(P(), P(DP_GROUP, None), P(DP_GROUP)),
        check_vma=False,
    )
```

```python
import jax
import jax.numpy as jnp
from jax import lax
from jax.experimental import pallas as pl
from jax.experimental.pallas import tpu as pltpu
from jax.sharding import Mesh
from jax.sharding import PartitionSpec as P


BINS = 4096
KEY_SHIFT = 18
DP = ("dp_0", "dp_1")
GROUP = ("group_0", "group_1")
DP_GROUP = ("dp_0", "dp_1", "group_0", "group_1")
LANES = 128
STEP = 64

SMEM = pltpu.MemorySpace.SMEM
VMEM = pltpu.MemorySpace.VMEM


def smem_spec():
    return pl.BlockSpec(memory_space=SMEM)


def any_spec():
    return pl.BlockSpec(memory_space=pltpu.MemorySpace.HBM)


def pack_rows(keys, dest, info, tokens, n_dev, n_member, slots):
    examples, width = tokens.shape
    tiles = width // LANES
    steps = examples // STEP
    n_owner = n_dev // n_member

    def kernel(keys_ref, dest_ref, info_ref, tok_ref, rows_ref, meta_ref, buf, seen, sent, sem):
        g = pl.program_id(0)

        @pl.when(g == 0)
        def _():
            sent[0] = 0
            for o in range(n_owner):
                seen[o] = 0

        @pl.when(g < steps)
        def _():
            for r in range(STEP // 8):
                for k in range(tiles):
                    at = (g * STEP + r * 8) * tiles + k
                    buf[pl.ds(at, 8, stride=tiles), :] = tok_ref[r * 8 : r * 8 + 8, k * LANES : (k + 1) * LANES]

        @pl.when(g > 0)
        def _():
            lowest = info_ref[0] << KEY_SHIFT

            def row(i, total):
                key = keys_ref[i]
                kept = key >= lowest

                @pl.when(kept)
                def _():
                    o = dest_ref[i]
                    local = seen[o]
                    seen[o] = local + 1
                    member = (info_ref[1 + o] + local) & (n_member - 1)
                    to = (o * n_member + member) * slots + local // n_member
                    meta_ref[to] = key
                    pltpu.make_async_copy(
                        buf.at[pl.ds(pl.multiple_of(i * tiles, tiles), tiles)],
                        rows_ref.at[pl.ds(pl.multiple_of(to * tiles, tiles), tiles)],
                        sem,
                    ).start()

                return total + kept.astype(jnp.int32)

            start = (g - 1) * STEP
            sent[0] = lax.fori_loop(start, start + STEP, row, sent[0])

        @pl.when(g == steps)
        def _():
            def drain(i, carry):
                pltpu.make_async_copy(buf.at[pl.ds(0, tiles)], rows_ref.at[pl.ds(0, tiles)], sem).wait()
                return carry

            lax.fori_loop(0, sent[0], drain, 0)

    return pl.pallas_call(
        kernel,
        grid=(steps + 1,),
        in_specs=[
            smem_spec(),
            smem_spec(),
            smem_spec(),
            pl.BlockSpec((STEP, width), lambda g: (jnp.minimum(g, steps - 1), 0)),
        ],
        out_specs=[any_spec(), smem_spec()],
        out_shape=[
            jax.ShapeDtypeStruct((n_dev * slots * tiles, LANES), tokens.dtype),
            jax.ShapeDtypeStruct((n_dev * slots,), keys.dtype),
        ],
        scratch_shapes=[
            pltpu.VMEM((examples * tiles, LANES), tokens.dtype),
            pltpu.SMEM((n_owner,), jnp.int32),
            pltpu.SMEM((1,), jnp.int32),
            pltpu.SemaphoreType.DMA,
        ],
        name="pack_rows",
    )(keys, dest, info, tokens)


def incoming(counts_ref, member, n_dev, n_member, visit, carry):
    def source(s, state):
        before, carry = state
        count = counts_ref[s]
        first = (member - before) & (n_member - 1)
        rows = (count - first + n_member - 1) >> 3
        carry = visit(s, (before + first) >> 3, rows, carry)
        return before + count, carry

    return lax.fori_loop(0, n_dev, source, (0, carry))


def place_bins(counts, member, got_keys, n_dev, n_member, slots, capacity):
    def kernel(counts_ref, member_ref, keys_ref, out_ref):
        def clear(i, carry):
            for j in range(8):
                out_ref[i * 8 + j] = -1
            return carry

        lax.fori_loop(0, capacity // 8, clear, 0)

        def visit(s, slot, rows, carry):
            at = s * (slots * n_member) + ((member_ref[0] - carry) & (n_member - 1))

            def one(q, c):
                out_ref[slot + q] = keys_ref[at + q * n_member] >> KEY_SHIFT
                return c

            lax.fori_loop(0, rows, one, 0)
            return carry + counts_ref[s]

        incoming(counts_ref, member_ref[0], n_dev, n_member, visit, 0)

    return pl.pallas_call(
        kernel,
        in_specs=[smem_spec()] * 3,
        out_specs=smem_spec(),
        out_shape=jax.ShapeDtypeStruct((capacity,), jnp.int32),
        name="place_bins",
    )(counts, member, got_keys)


def unpack_rows(counts, member, got, n_dev, n_member, slots, capacity, width):
    tiles = width // LANES
    steps = capacity // STEP

    def kernel(counts_ref, member_ref, got_ref, out_ref, buf, pending, filled, sems):
        g = pl.program_id(0)

        @pl.when(g == 0)
        def _():
            for b in range(steps):
                pending[b] = 0

            def visit(s, slot, rows, carry):
                b = slot // STEP

                @pl.when(rows > 0)
                def _():
                    pending[b] = pending[b] + rows

                for n in range(1, slots + 1):

                    @pl.when(rows == n)
                    def _(n=n):
                        pltpu.make_async_copy(
                            got_ref.at[pl.ds(pl.multiple_of(s * (slots * tiles), tiles), n * tiles)],
                            buf.at[pl.ds(pl.multiple_of(slot * tiles, tiles), n * tiles)],
                            sems.at[b],
                        ).start()

                return carry

            total, _ = incoming(counts_ref, member_ref[0], n_dev, n_member, visit, 0)
            filled[0] = (total - member_ref[0] + n_member - 1) >> 3

        def drain(i, carry):
            pltpu.make_async_copy(got_ref.at[pl.ds(0, tiles)], buf.at[pl.ds(0, tiles)], sems.at[g]).wait()
            return carry

        lax.fori_loop(0, pending[g], drain, 0)
        index = g * STEP + lax.broadcasted_iota(jnp.int32, (8, LANES), 0)
        for r in range(STEP // 8):
            real = index + r * 8 < filled[0]
            for k in range(tiles):
                at = (g * STEP + r * 8) * tiles + k
                rows = buf[pl.ds(at, 8, stride=tiles), :]
                out_ref[r * 8 : r * 8 + 8, k * LANES : (k + 1) * LANES] = jnp.where(real, rows, 0)

    return pl.pallas_call(
        kernel,
        grid=(steps,),
        in_specs=[smem_spec(), smem_spec(), any_spec()],
        out_specs=pl.BlockSpec((STEP, width), lambda g: (g, 0)),
        out_shape=jax.ShapeDtypeStruct((capacity, width), got.dtype),
        scratch_shapes=[
            pltpu.VMEM((capacity * tiles, LANES), got.dtype),
            pltpu.SMEM((steps,), jnp.int32),
            pltpu.SMEM((1,), jnp.int32),
            pltpu.SemaphoreType.DMA((steps,)),
        ],
        name="unpack_rows",
    )(counts, member, got)


NEAR = 112
EDGES = (0, 56, 144, 216)
OWN = 128
PLACES = 2 * (NEAR + EDGES[-1]) + OWN


def segments(hop):
    return [(EDGES[j], EDGES[j + 1] - EDGES[j]) for j in range(min(3, 5 - hop))]


def pack_relay(source, tokens, offset, sizes):
    examples, width = tokens.shape
    tiles = width // LANES
    tiled = tokens.reshape(examples // 8, 8, tiles, LANES).transpose(0, 2, 1, 3)[..., None, :]
    parts = 4

    def kernel(source_ref, tok_ref, *rest):
        outs, (buf, sem_in, sem_out) = rest[: len(sizes)], rest[len(sizes) :]
        each = examples // 8 // parts
        loads = [
            pltpu.make_async_copy(tok_ref.at[pl.ds(i * each, each)], buf.at[pl.ds(i * each, each)], sem_in)
            for i in range(parts)
        ]
        for load in loads:
            load.start()
        for load in loads:
            load.wait()
        start = offset
        for out, size in zip(outs, sizes):

            def some(i, carry, out=out, start=start):
                for j in range(8):
                    row = source_ref[0, start + i * 8 + j]
                    pltpu.make_async_copy(slot_of(buf, row), out.at[i * 8 + j], sem_out).start()
                return carry

            lax.fori_loop(0, size // 8, some, 0)
            start += size
        for out in outs:
            pltpu.make_async_copy(out, out, sem_out).wait()

    packed = pl.pallas_call(
        kernel,
        in_specs=[smem_spec(), any_spec()],
        out_specs=[any_spec()] * len(sizes),
        out_shape=[jax.ShapeDtypeStruct((n, tiles, 1, LANES), tokens.dtype) for n in sizes],
        scratch_shapes=[
            pltpu.VMEM((examples // 8, tiles, 8, 1, LANES), tokens.dtype),
            pltpu.SemaphoreType.DMA,
            pltpu.SemaphoreType.DMA,
        ],
    )(source, tiled)
    return [rows.reshape(-1, LANES) for rows in packed]


ROUNDS = ((0, 1), (2,), (3, 4))


def lanes_of(hop):
    if hop == 0:
        return [((0,), 4)]
    if hop == 4:
        return [((0, 1), 4)]
    return [((0,), 4), ((1,), 4)]


def slot_map():
    found = {}
    for n, hops in enumerate(ROUNDS):
        skip = 0
        for hop in hops:
            for sides, slots in lanes_of(hop):
                for side in sides:
                    found[hop if side == 0 else (8 - hop) % 8] = (n, skip)
                skip += slots
        for d, (m, at) in list(found.items()):
            if m == n and not isinstance(at, tuple):
                found[d] = (m, (at, skip))
    return {d: (n, rows, at) for d, (n, (at, rows)) in found.items()}


def spread(n, place, counts, befores, pieces, n_member, tiles, onto=None):
    slots = slot_map()
    width = next(rows for m, rows, _ in slots.values() if m == n)
    total = 4 * n_member * width * tiles
    origins, held = {}, 0
    for hop, side, start, rows, _ in pieces:
        if (hop, side) not in origins:
            rows_in = (OWN, NEAR, EDGES[3], EDGES[2], EDGES[1])[hop]
            origins[hop, side] = (held, rows_in)
            held += rows_in + 32
    arrays = [array for *_, array in pieces]
    laid = sum(4 * (16 if hop == 4 else 32) for hop, _ in origins)
    base_of = [] if onto is None else [onto]

    def kernel(place_ref, counts_ref, befores_ref, *rest):
        rest = rest[len(base_of) :]
        ins, (out, buf, sem_in, sem_out) = rest[: len(pieces)], rest[len(pieces) :]
        loads = []
        for (hop, side, start, rows, _), ref in zip(pieces, ins):
            at = (origins[hop, side][0] + start) * tiles
            loads.append(pltpu.make_async_copy(ref, buf.at[pl.ds(at, rows * tiles)], sem_in))
        for load in loads:
            load.start()
        z = place_ref[0]
        todo = []
        for (hop, side), (base, rows_in) in origins.items():
            sign = 1 - 2 * side
            origin = (z - sign * hop) & 7

            def share(y, k, origin=origin, sign=sign, side=side):
                count = counts_ref[origin * 32 + y * 8 + ((origin + sign * k) & 7)]
                return (count + 1 - side) >> 1 if k == 4 else count

            at = 0
            if hop > 1:
                for k in range(hop + 1, 5):
                    for y in range(4):
                        at += share(y, k)
            for y in range(4):
                todo.append((hop, side, y, base + jnp.minimum(at, rows_in), befores_ref[origin * 32 + y * 8 + z]))
                at += share(y, hop)
        for load in loads:
            load.wait()
        for hop, side, y, first, before in todo:
            skip = slots[hop if side == 0 else (8 - hop) % 8][2]
            for j in range(16 if hop == 4 else 32):
                local = 2 * j + side if hop == 4 else j
                member = (before + local) & (n_member - 1)
                to = (y * n_member + member) * width + skip + local // n_member
                pltpu.make_async_copy(
                    buf.at[pl.ds(pl.multiple_of((first + j) * tiles, tiles), tiles)],
                    out.at[pl.ds(pl.multiple_of(to * tiles, tiles), tiles)],
                    sem_out,
                ).start()
        whole = out.at[pl.ds(0, laid * tiles)]
        pltpu.make_async_copy(whole, whole, sem_out).wait()

    return pl.pallas_call(
        kernel,
        in_specs=[smem_spec()] * 3 + [any_spec()] * (len(base_of) + len(pieces)),
        out_specs=any_spec(),
        out_shape=jax.ShapeDtypeStruct((total, LANES), arrays[0].dtype),
        input_output_aliases={3: 0} if base_of else {},
        scratch_shapes=[
            pltpu.VMEM((held * tiles, LANES), arrays[0].dtype),
            pltpu.SemaphoreType.DMA,
            pltpu.SemaphoreType.DMA,
        ],
    )(place, counts, befores, *base_of, *arrays)


def copy_senders(d, slots_of, place_ref, counts_ref, befores_ref, n_member, start):
    _, rows_each, skip = slots_of[d]
    member = place_ref[1]
    origin = (place_ref[0] - d) & 7

    def sender(i, total):
        s = ((i >> 3) * 8 + origin) * n_member + (i & 7)
        before = befores_ref[s]
        first = (member - before) & (n_member - 1)
        rows = (counts_ref[s] - first + n_member - 1) >> 3
        slot = (before + first) >> 3
        for q in range(4):

            @pl.when(q < rows)
            def _(q=q):
                start(i * rows_each + skip + q, slot + q)

        return total + rows

    return lax.fori_loop(0, 4 * n_member, sender, 0)


def slot_of(ref, slot):
    return ref.at[slot >> 3, :, slot & 7]


def unpack_early(place, counts, befores, got, n_member, capacity, tiles):
    slots_of = slot_map()
    groups = capacity // 8

    def kernel(place_ref, counts_ref, befores_ref, *rest):
        ins, (out_ref, buf, zero, sem_in, sem_out) = rest[: len(got)], rest[len(got) :]
        zero[...] = jnp.zeros(zero.shape, zero.dtype)
        moved = 0
        for d in range(8):
            n = slots_of[d][0]
            if n < len(got):

                def start(row, slot, n=n):
                    pltpu.make_async_copy(ins[n].at[row], slot_of(buf, slot), sem_in).start()

                moved += copy_senders(d, slots_of, place_ref, counts_ref, befores_ref, n_member, start)

        def drain(i, carry):
            pltpu.make_async_copy(ins[0].at[0], buf.at[0, :, 0], sem_in).wait()
            return carry

        lax.fori_loop(0, moved, drain, 0)
        end = 32 * n_member - 1
        filled = (befores_ref[end] + counts_ref[end] - place_ref[1] + n_member - 1) >> 3
        whole, extra = filled >> 3, filled & 7

        def group(g, carry):
            @pl.when(g < whole)
            def _():
                pltpu.make_async_copy(buf.at[g], out_ref.at[g], sem_out).start()

            @pl.when((g > whole) | ((g == whole) & (extra == 0)))
            def _():
                pltpu.make_async_copy(zero, out_ref.at[g], sem_out).start()

            @pl.when((g == whole) & (extra > 0))
            def _():
                for k in range(8):

                    @pl.when(k < extra)
                    def _(k=k):
                        pltpu.make_async_copy(buf.at[g, :, k], out_ref.at[g, :, k], sem_out).start()

                    @pl.when(k >= extra)
                    def _(k=k):
                        pltpu.make_async_copy(zero.at[:, k], out_ref.at[g, :, k], sem_out).start()

            return carry

        lax.fori_loop(0, groups, group, 0)
        pltpu.make_async_copy(buf, out_ref, sem_out).wait()

    return pl.pallas_call(
        kernel,
        in_specs=[smem_spec()] * 3 + [any_spec()] * len(got),
        out_specs=any_spec(),
        out_shape=jax.ShapeDtypeStruct((groups, tiles, 8, 1, LANES), got[0].dtype),
        scratch_shapes=[
            pltpu.VMEM((groups, tiles, 8, 1, LANES), got[0].dtype),
            pltpu.VMEM((tiles, 8, 1, LANES), got[0].dtype),
            pltpu.SemaphoreType.DMA,
            pltpu.SemaphoreType.DMA,
        ],
        name="unpack_early",
    )(place, counts, befores, *got)


def unpack_last(place, counts, befores, early, last, n_member):
    slots_of = slot_map()
    late = [d for d in range(8) if slots_of[d][0] == len(ROUNDS) - 1]
    last = pltpu.with_memory_space_constraint(last, pltpu.MemorySpace.VMEM)

    def kernel(place_ref, counts_ref, befores_ref, early_ref, buf, out_ref, sem_out):

        def start(row, slot):
            pltpu.make_async_copy(buf.at[row], slot_of(out_ref, slot), sem_out).start()

        moved = 0
        for d in late:
            moved += copy_senders(d, slots_of, place_ref, counts_ref, befores_ref, n_member, start)

        def drain(i, carry):
            pltpu.make_async_copy(buf.at[0], out_ref.at[0, :, 0], sem_out).wait()
            return carry

        lax.fori_loop(0, moved, drain, 0)

    return pl.pallas_call(
        kernel,
        in_specs=[smem_spec()] * 3 + [any_spec(), pl.BlockSpec(memory_space=pltpu.MemorySpace.VMEM)],
        out_specs=any_spec(),
        out_shape=jax.ShapeDtypeStruct(early.shape, early.dtype),
        input_output_aliases={3: 0},
        scratch_shapes=[pltpu.SemaphoreType.DMA],
        name="unpack_last",
    )(place, counts, befores, early, last)


def plan_relay(keys, dest, cut, z, tokens):
    examples = keys.shape[1]
    padded = -(-PLACES // LANES) * LANES
    tiles = tokens.shape[1] // LANES
    tiled = tokens.reshape(examples // 8, 8, tiles, LANES).transpose(0, 2, 1, 3)[..., None, :]

    def across(left, right):
        return lax.dot_general(left, right, (((1,), (1,)), ((), ())), preferred_element_type=jnp.float32)

    def kernel(
        keys_ref, dest_ref, cut_ref, z_ref, tok_ref, plan_ref, rank_ref, counts_ref, up_ref, down_ref,
        buf, source, sem_in, sem_plan, sem_out,
    ):
        load = pltpu.make_async_copy(tok_ref, buf, sem_in)
        load.start()
        kept = (keys_ref[...] >> KEY_SHIFT) >= cut_ref[0]
        owner = lax.broadcasted_iota(jnp.int32, (32, examples), 0)
        hot = (dest_ref[...] == owner) & kept
        ones = jnp.where(hot, 1.0, 0.0).astype(jnp.bfloat16)
        row = lax.broadcasted_iota(jnp.int32, (examples, examples), 0)
        col = lax.broadcasted_iota(jnp.int32, (examples, examples), 1)
        before = jnp.where(row < col, 1.0, 0.0).astype(jnp.bfloat16)
        running = jnp.dot(ones, before, preferred_element_type=jnp.float32).astype(jnp.int32)
        counts = across(jnp.ones((8, examples), jnp.bfloat16), ones).astype(jnp.int32)[0:1, :]
        counts_ref[...] = counts
        rank_ref[...] = jnp.sum(jnp.where(hot, running, 0), axis=0, keepdims=True)

        z = z_ref[0]

        def about(axis):
            o = lax.broadcasted_iota(jnp.int32, (32, 32), axis)
            d = ((o & 7) - z) & 7
            dist = jnp.minimum(d, 8 - d)
            far = jnp.where(dist > 1, 1, 0)
            return d, dist, far * 64 + (4 - dist) * 4 + (o >> 3), far

        d, dist, order, far = about(0)
        d_of, _, order_of, far_of = about(1)
        earlier = (order_of < order) & (far_of == far)

        def start(members, sizes):
            return jnp.sum(jnp.where(earlier & members, sizes, 0), axis=1, keepdims=True)

        start_ahead = start((d_of >= 1) & (d_of <= 4), jnp.where(d_of == 4, (counts + 1) >> 1, counts))
        start_back = start(d_of >= 4, jnp.where(d_of == 4, counts >> 1, counts))
        start_own = start(d_of == 0, jnp.broadcast_to(counts, (32, 32)))
        d, dist = d[:, 0:1], dist[:, 0:1]
        ahead = (d >= 1) & (d <= 4)
        far_ahead, far_back, mine = 2 * NEAR, 2 * NEAR + EDGES[-1], 2 * NEAR + 2 * EDGES[-1]
        first = jnp.where(
            d == 0, mine, jnp.where(ahead, jnp.where(d == 1, 0, far_ahead), jnp.where(d == 7, NEAR, far_back))
        )
        base = first + jnp.where(d == 0, start_own, jnp.where(ahead, start_ahead, start_back))
        other = far_back + start_back
        limit = first + jnp.where(d == 0, OWN, jnp.where(dist == 1, NEAR, EDGES[-1]))
        odd = (d == 4) & ((running & 1) == 1)
        position = jnp.where(odd, other, base) + jnp.where(d == 4, running >> 1, running)
        bound = jnp.where(odd, mine, limit)
        position = jnp.sum(jnp.where(hot & (position < bound), position + 1, 0), axis=0, keepdims=True) - 1

        place = lax.broadcasted_iota(jnp.int32, (padded, examples), 0)
        here = jnp.where(place == position, 1.0, 0.0).astype(jnp.bfloat16)
        part = lax.broadcasted_iota(jnp.int32, (8, examples), 0)
        example = lax.broadcasted_iota(jnp.int32, (8, examples), 1)
        parts = jnp.where(part == 0, example >> 4, jnp.where(part == 1, example & 15, 0))
        found = across(parts.astype(jnp.float32).astype(jnp.bfloat16), here).astype(jnp.int32)
        plan_ref[...] = found[0:1, :] * 16 + found[1:2, :]
        load.wait()
        move = pltpu.make_async_copy(plan_ref, source, sem_plan)
        move.start()
        move.wait()
        for out, start in ((up_ref, 0), (down_ref, NEAR)):

            def some(i, carry, out=out, start=start):
                for j in range(8):
                    row = source[0, start + i * 8 + j]
                    pltpu.make_async_copy(slot_of(buf, row), out.at[i * 8 + j], sem_out).start()
                return carry

            lax.fori_loop(0, NEAR // 8, some, 0)
        for out in (up_ref, down_ref):
            pltpu.make_async_copy(out, out, sem_out).wait()

    whole = pl.BlockSpec(memory_space=VMEM)
    return pl.pallas_call(
        kernel,
        in_specs=[whole, whole, smem_spec(), smem_spec(), any_spec()],
        out_specs=[whole] * 3 + [any_spec()] * 2,
        out_shape=[
            jax.ShapeDtypeStruct((1, padded), jnp.int32),
            jax.ShapeDtypeStruct((1, examples), jnp.int32),
            jax.ShapeDtypeStruct((1, 32), jnp.int32),
            *[jax.ShapeDtypeStruct((NEAR, tiles, 1, LANES), tokens.dtype)] * 2,
        ],
        scratch_shapes=[
            pltpu.VMEM(tiled.shape, tokens.dtype),
            pltpu.SMEM((1, padded), jnp.int32),
            *[pltpu.SemaphoreType.DMA] * 3,
        ],
        name="plan_relay",
    )(keys, dest, cut, z, tiled)


def by_owner(values, position, size):
    places = jnp.arange(size, dtype=jnp.int32)
    return jnp.sum(jnp.where(position[None, :] == places[:, None], values[None, :], 0), axis=1)


def relay_fits(table):
    n_dev = table.shape[0]
    z = (jnp.arange(n_dev, dtype=jnp.int32)[:, None] // 8) % 8
    d = (jnp.arange(32, dtype=jnp.int32)[None, :] - z) % 8
    plus = jnp.where(d == 4, (table + 1) >> 1, table)
    minus = jnp.where(d == 4, table >> 1, table)
    over = jnp.zeros((), jnp.int32)
    for least, most, cap in ((1, 1, NEAR), (2, 4, EDGES[3]), (3, 4, EDGES[2]), (4, 4, EDGES[1])):
        ahead = jnp.sum(jnp.where((d >= least) & (d <= most), plus, 0), axis=1)
        back = jnp.sum(jnp.where((d <= 8 - least) & (d >= 8 - most), minus, 0), axis=1)
        over = jnp.maximum(over, jnp.max(jnp.maximum(ahead, back)) - cap)
    return over <= 0


def exchange(value, axes=DP_GROUP):
    return lax.all_to_all(value, axes, split_axis=0, concat_axis=0, tiled=True)


def hop_on(value, step, axis="dp_1"):
    count = lax.axis_size(axis)
    return lax.ppermute(value, axis, [(i, (i + step) % count) for i in range(count)])


DOUBLING = (
    ("group_1", 1), ("group_0", 1), ("group_0", 2), ("dp_0", 1), ("dp_0", 2), ("dp_1", 1), ("dp_1", 2), ("dp_1", 4),
)


def program(keys, cut, owner, tokens):
    examples = keys.shape[0]
    width = tokens.shape[1]
    tiles = width // LANES
    n_owner = lax.axis_size(DP)
    n_member = lax.axis_size(GROUP)
    n_dev = n_owner * n_member
    slots = 2 * examples // n_dev
    capacity = 2 * examples
    most = slots * n_member
    me = lax.axis_index(DP_GROUP)
    member = lax.axis_index(GROUP)
    y, z = lax.axis_index("dp_0"), lax.axis_index("dp_1")
    bins_of = keys >> KEY_SHIFT
    dest = owner[:, 0]
    kept = bins_of >= cut[0]
    source, local_rank, counts, *near = plan_relay(
        keys[None, :], owner.reshape(1, -1), cut, z[None].astype(jnp.int32), tokens
    )
    near = [rows.reshape(-1, LANES) for rows in near]
    local_rank, counts = local_rank[0], counts[0]
    *far, own = pack_relay(source, tokens, 2 * NEAR, [n for _, n in segments(1)] * 2 + [OWN])
    plus, minus = far[:3], far[3:]

    hist = jnp.zeros((BINS,), jnp.int32).at[bins_of].add(1)
    for axis, step in DOUBLING:
        hist = hist + hop_on(hist, step, axis)
    own_keys = by_owner(keys, jnp.where(kept, dest * most + local_rank, -1), n_owner * most).reshape(n_owner, 1, most)
    own_keys = jnp.broadcast_to(own_keys, (n_owner, n_member, most)).reshape(n_dev, most)
    first = jnp.concatenate([jnp.broadcast_to(counts[None, :], (n_dev, n_owner)), own_keys], axis=1)
    first, _ = lax.optimization_barrier((first, source))
    first = exchange(first)
    table = first[:, :n_owner]
    got_keys = first[:, n_owner:].reshape(-1)
    device = jnp.arange(n_dev, dtype=jnp.int32)
    below = (device[None, :] < device[:, None]).astype(jnp.bfloat16)
    befores = jnp.dot(below, table.astype(jnp.bfloat16), preferred_element_type=jnp.float32).astype(jnp.int32)
    before = lax.dynamic_slice_in_dim(befores, me, 1, axis=0)[0]

    def column(values):
        return lax.dynamic_slice_in_dim(values, me // n_member, 1, axis=1)[:, 0]

    def line(values):
        return lax.dynamic_slice(values.reshape(4, 8, n_member, n_owner), (y, 0, member, 0), (1, 8, 1, n_owner)).reshape(-1)

    mine, mine_before = column(table), column(befores)
    line_counts, line_befores = line(table), line(befores)
    fits = relay_fits(table)
    place = jnp.stack([z, member]).astype(jnp.int32)

    slot_bins = place_bins(mine, member[None], got_keys, n_dev, n_member, slots, capacity)

    arrived = {0: [(0, 0, 0, OWN, own)]}
    near = [hop_on(near[0], 1), hop_on(near[1], -1)]
    arrived[1] = [(1, i, 0, NEAR, v) for i, v in enumerate(near)]
    for k in range(1, 5):
        spans = segments(k)
        plus = [hop_on(v, 1) for v in plus[: len(spans)]]
        minus = [hop_on(v, -1) for v in minus[: len(spans)]]
        if k > 1:
            arrived[k] = [(k, i, *span, v) for i, side in enumerate((plus, minus)) for span, v in zip(spans, side)]
    got = []
    for n, hops in enumerate(ROUNDS):
        calls = [[k] for k in hops] if hops[-1] == 4 else [hops]
        laid = None
        for ks in calls:
            laid = spread(n, place, line_counts, line_befores, [p for k in ks for p in arrived[k]], n_member, tiles, laid)
        laid = laid.reshape(n_owner, -1, tiles, LANES)
        if n > 0:
            laid, got[-1] = lax.optimization_barrier((laid, got[-1]))
        got.append(exchange(laid, ("dp_0",) + GROUP).reshape(-1, tiles, 1, LANES))

    early = unpack_early(place, mine, mine_before, got[:-1], n_member, capacity, tiles)
    packed = unpack_last(place, mine, mine_before, early, got[-1], n_member)
    packed = packed.reshape(capacity // 8, tiles, 8, LANES).transpose(0, 2, 1, 3).reshape(capacity, width)

    def direct(state):
        info = jnp.concatenate([cut, before])
        send_rows, _ = pack_rows(keys, dest, info, tokens, n_dev, n_member, slots)
        rows = exchange(send_rows.reshape(n_dev, slots, tiles, LANES)).reshape(-1, LANES)
        return jnp.ones((), jnp.bool_), unpack_rows(mine, member[None], rows, n_dev, n_member, slots, capacity, width)

    _, packed = lax.while_loop(lambda state: ~state[0], direct, (fits, packed))

    suffix = jnp.cumsum(hist.astype(jnp.float32)[::-1])[::-1]
    total = jnp.maximum(suffix[cut[0]], 1.0)
    weights = jnp.where(slot_bins >= 0, suffix[jnp.maximum(slot_bins, 0)] / total, 0.0)
    return (hist, packed, weights)


def solution(mesh):
    torus = Mesh(mesh.devices.reshape(4, 8, 4, 2), ("dp_0", "dp_1", "group_0", "group_1"))
    placed = (P(DP_GROUP), P(), P(DP_GROUP, None), P(DP_GROUP, None))
    return jax.shard_map(
        program,
        mesh=torus,
        in_specs=placed,
        out_specs=(P(), P(DP_GROUP, None), P(DP_GROUP)),
        check_vma=False,
    )
```
